32 devices in a mesh: tab: 8 (over y, x, core), rep: 4 (over z).
Axes of the slice: x: 2, y: 2, z: 4, core: 2. Of those that a mesh axis runs over, the one named last changes fastest.
Arguments:
- pooled: bfloat16 [64, 4096, 128], P('tab', 'rep'), may hold values from -6 to 6
- widths: int32 [64], replicated, may hold values from 16 to 128, as said below
- placement: int32 [64], replicated, may hold values from 0 to 63, each once
- route: int32 [4, 1024], P('rep'), may hold values from 0 to 1023, each once within a row
- labels: int32 [4, 1024], P('rep'), may hold values 0 or 1
- proj: bfloat16 [64, 128, 32], replicated, may hold values from -0.5 to 0.5
- senet_in: float32 [64, 32], replicated, may hold values from -6 to 6
- senet_out: float32 [32, 64], replicated, may hold values from -1 to 1
- bilinear: float32 [32, 32], replicated, may hold values from -1 to 1
- w_first: bfloat16 [4096, 256], replicated, may hold values from -0.09375 to 0.09375
- w_second: bfloat16 [256, 256], replicated, may hold values from -0.75 to 0.75
- w_last: bfloat16 [256], replicated, may hold values from -0.375 to 0.375
Outputs:
- scores: float32 [4, 1024], P('rep', 'tab')
- d_pooled: bfloat16 [64, 4096, 128], P('tab', 'rep')
- d_proj: float32 [64, 128, 32], P('tab')
- d_senet_in: float32 [64, 32], replicated
- d_senet_out: float32 [32, 64], replicated
- d_bilinear: float32 [32, 32], replicated
- d_first: float32 [4096, 256], P('tab')
- d_second: float32 [256, 256], replicated
- d_last: float32 [256], replicated
The draws below stay inside these ranges and needn't reach their ends.
Inputs may be any that keep to these rules, and one draw needn't show every extreme that they name: `widths`: each field's width is 128, 64, 32 or 16. `placement`: a permutation of the fields. `route`: each row is a permutation of 0 to 1023.
All inputs are finite; a program needn't handle non-finite values. No bound on the sum of `labels` on one device may be relied on, other than what follows from the above.
Results may differ from the reference program's by a relative error of at most 0.017.
Values may be sent and summed in bfloat16 or wider, within the bound.
No kernel may reach another device: no remote copies, remote signals or barrier semaphores. Data moves between devices by JAX's collectives and lax.ppermute only.
A program may use at most 64 MiB of HBM per device.

```python
import jax
import jax.numpy as jnp
from jax import lax

F = 64
WMAX = 128
E = 32
R = 32
H = 256
B_DEV = 128
B_REP = 1024
BATCH = 4096
N_REP = 4


second_bound = 0.75


def draw_widths(key, part):
    levels = jax.random.randint(key, (F,), 0, 4)
    result = jnp.right_shift(jnp.full((F,), WMAX, jnp.int32), levels.astype(jnp.int32))
    chosen = jax.random.randint(jax.random.fold_in(key, 7), (), 0, F)
    return result.at[chosen].set(WMAX).astype(jnp.int32)


def draw_w_second(key, part):
    base = jax.random.uniform(jax.random.fold_in(key, 11), (H, H), jnp.float32, -second_bound, second_bound)
    result = base
    return result.astype(jnp.bfloat16)


def touch_ends(array, own_key, least, largest):
    extent = array.shape
    spot = [jax.random.randint(jax.random.fold_in(own_key, axis), (), 0, extent[axis]) for axis in range(len(extent))]
    array = array.at[tuple(spot)].set(least)
    longest = extent.index(max(extent))
    spot[longest] = (spot[longest] + 1) % extent[longest]
    return array.at[tuple(spot)].set(largest)


def shard_levels(rng, extent, shards, low, high):
    def one(position, blocks):
        draws = jax.random.uniform(jax.random.fold_in(jax.random.fold_in(rng, 6), position), (blocks,), jnp.float32, low / len(shards), high / len(shards))
        return jnp.repeat(jnp.exp(draws), extent[position] // blocks).reshape((-1,) + (1,) * (len(extent) - position - 1))

    gain = one(*shards[0])
    for cut in shards[1:]:
        gain = gain * one(*cut)
    return gain


def gaussian(key, extent, scale, bound, cuts=(), kind=jnp.bfloat16):
    factor_of = shard_levels(key, extent, cuts, -0.22, 0.18) if cuts else 1.0
    array = jax.random.normal(key, extent, jnp.float32) * scale * factor_of
    return jnp.minimum(jnp.maximum(array, -bound), bound).astype(kind)


def setup_inputs(seed: int = 0) -> dict:
    key_list = jax.random.split(jax.random.key(seed), 13)
    pooled = gaussian(key_list[0], (F, BATCH, WMAX), 1.0, 6.0, ((0, 8), (1, 4)))
    widths = draw_widths(jax.random.fold_in(key_list[12], 71), 0)
    placement = jax.random.permutation(key_list[2], F).astype(jnp.int32)
    route = jax.vmap(lambda own: jax.random.permutation(own, B_REP))(jax.random.split(key_list[3], N_REP)).reshape((N_REP, B_REP)).astype(jnp.int32)
    labels = touch_ends((jax.random.randint(key_list[4], (N_REP, B_REP), 0, 4) < 1).astype(jnp.int32), jax.random.fold_in(key_list[4], 1), 0, 1)
    proj = gaussian(key_list[5], (F, WMAX, E), WMAX ** -0.5, 0.5)
    senet_in = gaussian(key_list[6], (F, R), 1.0, 6.0, (), jnp.float32)
    senet_out = gaussian(key_list[7], (R, F), R ** -0.5, 1.0, (), jnp.float32)
    bilinear = gaussian(key_list[8], (E, E), E ** -0.5, 1.0, (), jnp.float32)
    w_first = gaussian(key_list[9], (2 * F * E, H), (2 * F * E) ** -0.5, 0.09375)
    w_second = draw_w_second(jax.random.fold_in(key_list[12], 71), 0)
    w_last = gaussian(key_list[11], (H,), H ** -0.5, 0.375)
    return {"pooled": pooled, "widths": widths, "placement": placement, "route": route, "labels": labels, "proj": proj, "senet_in": senet_in, "senet_out": senet_out, "bilinear": bilinear, "w_first": w_first, "w_second": w_second, "w_last": w_last}


PRECISE = lax.Precision.HIGHEST


def silu_slope(pre_act):
    logistic = jax.nn.sigmoid(pre_act)
    return logistic * (1.0 + pre_act * (1.0 - logistic))


def bilinear_forward(fields_in, bilinear, factor):
    product = jnp.einsum("fnc,cd->fnd", fields_in, bilinear, precision=PRECISE)
    others = jnp.sum(fields_in, axis=0, keepdims=True) - fields_in
    return product * others * factor, product, others


def bilinear_backward(fields_in, product, others, upstream, bilinear, factor):
    d_product = upstream * others * factor
    d_others = upstream * product * factor
    d_fields = jnp.einsum("fnd,cd->fnc", d_product, bilinear, precision=PRECISE)
    d_fields = d_fields + jnp.sum(d_others, axis=0, keepdims=True) - d_others
    d_weight = jnp.einsum("fnc,fnd->cd", fields_in, d_product, precision=PRECISE)
    return d_fields, d_weight


def owner_pass(embeds, targets, senet_in, senet_out, bilinear, w_first, w_second, w_last):
    count = embeds.shape[0]
    width = embeds.shape[2]
    hidden = w_second.shape[0]
    factor = count ** -0.5
    first = w_first.reshape(2, count, width, hidden).astype(jnp.float32)
    dense = embeds.astype(jnp.float32)
    squeeze = jnp.mean(dense, axis=2)
    pre_one = jnp.einsum("fn,fr->rn", squeeze, senet_in, precision=PRECISE)
    act_one = jax.nn.silu(pre_one)
    pre_two = jnp.einsum("rn,rf->fn", act_one, senet_out, precision=PRECISE)
    weights = jax.nn.sigmoid(pre_two)
    scaled = weights[:, :, None] * dense
    plain_out, plain_prod, plain_rest = bilinear_forward(dense, bilinear, factor)
    scaled_out, scaled_prod, scaled_rest = bilinear_forward(scaled, bilinear, factor)
    joined = jnp.stack([plain_out, scaled_out]).astype(jnp.bfloat16)
    joined_wide = joined.astype(jnp.float32)
    pre_hidden = jnp.einsum("kfnc,kfch->nh", joined_wide, first, precision=PRECISE)
    hidden_one = jax.nn.silu(pre_hidden).astype(jnp.bfloat16)
    pre_second = jnp.dot(hidden_one, w_second, preferred_element_type=jnp.float32)
    hidden_two = jax.nn.silu(pre_second).astype(jnp.bfloat16)
    logits = jnp.dot(hidden_two, w_last, preferred_element_type=jnp.float32)
    grad_logit = jax.nn.sigmoid(logits) - targets
    d_last = jnp.dot(grad_logit, hidden_two.astype(jnp.float32), precision=PRECISE)
    last_wide = w_last.astype(jnp.float32)
    d_pre_two = (grad_logit[:, None] * last_wide[None, :] * silu_slope(pre_second)).astype(jnp.bfloat16)
    d_second = jnp.dot(hidden_one.T, d_pre_two, preferred_element_type=jnp.float32)
    back_two = jnp.dot(d_pre_two, w_second.T, preferred_element_type=jnp.float32)
    d_pre_one = (back_two * silu_slope(pre_hidden)).astype(jnp.bfloat16)
    d_pre_wide = d_pre_one.astype(jnp.float32)
    d_first = jnp.einsum("kfnc,nh->kfch", joined_wide, d_pre_wide, precision=PRECISE).reshape(-1, hidden)
    d_joined = jnp.einsum("nh,kfch->kfnc", d_pre_wide, first, precision=PRECISE)
    d_plain, d_bil_plain = bilinear_backward(dense, plain_prod, plain_rest, d_joined[0], bilinear, factor)
    d_scaled, d_bil_scaled = bilinear_backward(scaled, scaled_prod, scaled_rest, d_joined[1], bilinear, factor)
    d_weights = jnp.sum(d_scaled * dense, axis=2)
    d_pre_w = d_weights * weights * (1.0 - weights)
    d_senet_out = jnp.einsum("rn,fn->rf", act_one, d_pre_w, precision=PRECISE)
    d_act = jnp.einsum("fn,rf->rn", d_pre_w, senet_out, precision=PRECISE) * silu_slope(pre_one)
    d_senet_in = jnp.einsum("fn,rn->fr", squeeze, d_act, precision=PRECISE)
    d_squeeze = jnp.einsum("rn,fr->fn", d_act, senet_in, precision=PRECISE)
    d_embeds = d_plain + weights[:, :, None] * d_scaled + d_squeeze[:, :, None] / width
    small = (d_senet_in, d_senet_out, d_bil_plain + d_bil_scaled, d_second, d_last)
    return logits, d_embeds.astype(jnp.bfloat16), small, d_first


def reference(pooled, widths, placement, route, labels, proj, senet_in, senet_out, bilinear, w_first, w_second, w_last):
    total = pooled.shape[1]
    padded = pooled.shape[2]
    field_count = placement.shape[0]
    ids = jnp.arange(field_count, dtype=jnp.int32)
    slot_width = widths[placement]
    slot_mask = (jnp.arange(padded, dtype=jnp.int32)[None, :] < slot_width[:, None]).astype(pooled.dtype)
    slot_proj = proj[placement].astype(jnp.float32)
    inverse = jnp.zeros_like(placement).at[placement].set(ids)
    flat_labels = labels.reshape(-1).astype(jnp.float32)
    block = B_DEV * N_REP
    turns = total // block
    hidden = w_second.shape[0]
    width = proj.shape[2]
    senet_rows = senet_in.shape[1]

    def one_block(index, carry):
        grads_pooled, logits_all, sums, first_sum = carry
        start = (index * block).astype(jnp.int32)
        rows = lax.dynamic_slice_in_dim(pooled, start, block, 1)
        masked = rows * slot_mask[:, None, :]
        embed_slot = jnp.einsum("fnc,fcd->fnd", masked.astype(jnp.float32), slot_proj, precision=PRECISE).astype(jnp.bfloat16)
        embed_field = embed_slot[inverse]
        targets = lax.dynamic_slice_in_dim(flat_labels, start, block)
        logits, d_embeds, small, d_first = owner_pass(embed_field, targets, senet_in, senet_out, bilinear, w_first, w_second, w_last)
        d_slot = d_embeds[placement].astype(jnp.float32)
        back = jnp.einsum("fnd,fcd->fnc", d_slot, slot_proj, precision=PRECISE)
        back = (back * slot_mask[:, None, :].astype(jnp.float32)).astype(pooled.dtype)
        d_proj_part = jnp.einsum("fnc,fnd->fcd", masked.astype(jnp.float32), d_slot, precision=PRECISE)
        grads_pooled = lax.dynamic_update_slice_in_dim(grads_pooled, back, start, 1)
        logits_all = lax.dynamic_update_slice_in_dim(logits_all, logits, start, 0)
        parts = (d_proj_part,) + small
        sums = tuple(old + new for old, new in zip(sums, parts))
        return grads_pooled, logits_all, sums, first_sum + d_first

    start_sums = (
        jnp.zeros((field_count, padded, width), jnp.float32),
        jnp.zeros((field_count, senet_rows), jnp.float32),
        jnp.zeros((senet_rows, field_count), jnp.float32),
        jnp.zeros((width, width), jnp.float32),
        jnp.zeros((hidden, hidden), jnp.float32),
        jnp.zeros((hidden,), jnp.float32),
    )
    start = (jnp.zeros_like(pooled), jnp.zeros((total,), jnp.float32), start_sums, jnp.zeros(w_first.shape, jnp.float32))
    grads_pooled, logits_all, sums, first_sum = lax.fori_loop(0, turns, one_block, start)
    scores = jnp.take_along_axis(logits_all.reshape(N_REP, B_REP), route, axis=1)
    d_proj, d_senet_in, d_senet_out, d_bilinear, d_second, d_last = sums
    return scores, grads_pooled, d_proj, d_senet_in, d_senet_out, d_bilinear, first_sum, d_second, d_last
```

```python
import functools

import jax
import jax.numpy as jnp
from jax import lax
from jax.experimental import pallas as pl
from jax.experimental.pallas import tpu as pltpu
from jax.sharding import PartitionSpec as P


PRECISE = lax.Precision.HIGHEST
BF = jnp.bfloat16
F32 = jnp.float32
VMEM = pltpu.VMEM
NN = (((1,), (0,)), ((), ()))
NT = (((1,), (1,)), ((), ()))
TN = (((0,), (0,)), ((), ()))


def dot(a, b, dims=NN, precision=None):
    return lax.dot_general(a, b, dims, precision=precision, preferred_element_type=F32)


def split(x):
    high = x.astype(BF)
    return high, (x - high.astype(F32)).astype(BF)


def silu_slope(pre_act):
    logistic = jax.nn.sigmoid(pre_act)
    return logistic * (1.0 + pre_act * (1.0 - logistic))


def vspec():
    return pl.BlockSpec(memory_space=VMEM)


def hspec():
    return pl.BlockSpec(memory_space=pltpu.HBM)


def far(*arrays):
    return tuple(pltpu.with_memory_space_constraint(a, pltpu.HBM) for a in arrays)


def params(mebibytes):
    return pltpu.CompilerParams(vmem_limit_bytes=mebibytes << 20)


def embed_body(widths_hbm, placement_hbm, pooled, proj, out, weight_out, widths, placement, rows_in, gathered, weights, staged, sems, table_sems, out_sems):
    slots, _, padded = rows_in.shape
    width = proj.shape[1]
    tab, _, owner = staged.shape
    first = lax.axis_index("tab") * slots
    tables = [
        pltpu.make_async_copy(placement_hbm, placement, table_sems.at[0]),
        pltpu.make_async_copy(widths_hbm, widths, table_sems.at[1]),
    ]
    for copy in tables:
        copy.start()
    large = [pltpu.make_async_copy(pooled.at[s], rows_in.at[s], sems.at[0, s]) for s in range(slots)]
    for copy in large:
        copy.start()
    for copy in tables:
        copy.wait()
    small = [pltpu.make_async_copy(proj.at[placement[first + s]], gathered.at[s], sems.at[1, s]) for s in range(slots)]
    for copy in small:
        copy.start()
    lane = lax.broadcasted_iota(jnp.int32, (width, padded), 1)
    gone = []
    for s in range(slots):
        part = slice(s * width, (s + 1) * width)
        keep = lane < widths[placement[first + s]]
        small[s].wait()
        weight = jnp.where(keep, gathered[s].astype(F32), 0.0).astype(BF)
        weights[part, :] = weight
        large[s].wait()
        embeds = dot(weight, rows_in[s], NT).astype(BF)
        for o in range(tab):
            staged[o, part, :] = embeds[:, o * owner : (o + 1) * owner]
        copy = pltpu.make_async_copy(staged.at[:, part, :], out.at[:, part, :], out_sems.at[s])
        copy.start()
        gone.append(copy)
    copy = pltpu.make_async_copy(weights, weight_out, table_sems.at[0])
    copy.start()
    gone.append(copy)
    for copy in gone:
        copy.wait()


def embed_slots(widths, placement, pooled, proj, tab):
    slots, rows, padded = pooled.shape
    width = proj.shape[1]
    fields = placement.shape[0]
    return pl.pallas_call(
        embed_body,
        out_shape=(
            pltpu.HBM((tab, slots * width, rows // tab), BF),
            pltpu.HBM((slots * width, padded), BF),
        ),
        in_specs=[hspec()] * 4,
        out_specs=(hspec(), hspec()),
        scratch_shapes=[
            pltpu.SMEM((fields,), jnp.int32),
            pltpu.SMEM((fields,), jnp.int32),
            pltpu.VMEM((slots, rows, padded), BF),
            pltpu.VMEM((slots, width, padded), BF),
            pltpu.VMEM((slots * width, padded), BF),
            pltpu.VMEM((tab, slots * width, rows // tab), BF),
            pltpu.SemaphoreType.DMA((2, slots)),
            pltpu.SemaphoreType.DMA((2,)),
            pltpu.SemaphoreType.DMA((slots,)),
        ],
        compiler_params=params(12),
        name="embed_slots",
    )(*far(widths, placement, pooled, proj))


def prepare_body(order, first_hbm, second_hbm, bilinear_hbm, last_hbm, *rest):
    outs, (first, second, bilinear, last), made, sems, out_sems = rest[:6], rest[6:10], rest[10:16], rest[16], rest[17]
    first_turned, second_turned, kron_high, kron_low, back_high, last_column = made
    copies = [
        pltpu.make_async_copy(source, target, sems.at[i])
        for i, (source, target) in enumerate(
            ((bilinear_hbm, bilinear), (last_hbm, last), (second_hbm, second), (first_hbm, first))
        )
    ]
    for copy in copies:
        copy.start()
    leaving = [pltpu.make_async_copy(made[i], outs[i], out_sems.at[i]) for i in range(len(outs))]
    width = bilinear.shape[0]
    side = kron_high.shape[0]
    copies[0].wait()
    tiled = jnp.concatenate([bilinear[...]] * (side // width), axis=1)
    tiled = jnp.concatenate([tiled] * (side // width), axis=0)
    row = lax.broadcasted_iota(jnp.int32, (side, side), 0) // width
    column = lax.broadcasted_iota(jnp.int32, (side, side), 1) // width
    kron = jnp.where(row == column, tiled, 0.0)
    back_high[...] = kron.astype(BF)
    kron_high[...], kron_low[...] = split(kron.T)
    hidden = last.shape[1]
    row = lax.broadcasted_iota(jnp.int32, (hidden, hidden), 0)
    column = lax.broadcasted_iota(jnp.int32, (hidden, hidden), 1)
    copies[1].wait()
    last_column[...] = jnp.sum(jnp.where(row == column, last[...].astype(F32), 0.0), axis=1, keepdims=True)
    copies[2].wait()
    second_turned[...] = second[...].T
    for copy in leaving[1:]:
        copy.start()
    copies[3].wait()
    step = min(512, first.shape[0])
    for g in range(0, first.shape[0], step):
        first_turned[:, g : g + step] = first[g : g + step, :].T
    leaving[0].start()
    for copy in leaving:
        copy.wait()


def prepare(order, w_first, w_second, bilinear, w_last):
    total, hidden = w_first.shape
    side = min(256, total)
    shapes = (
        ((hidden, total), BF), ((hidden, hidden), BF), ((side, side), BF), ((side, side), BF), ((side, side), BF),
        ((hidden, 1), F32),
    )
    return pl.pallas_call(
        prepare_body,
        out_shape=tuple(pltpu.HBM(s, d) for s, d in shapes),
        in_specs=[hspec()] * 5,
        out_specs=tuple(hspec() for _ in shapes),
        scratch_shapes=[
            pltpu.VMEM(w_first.shape, BF),
            pltpu.VMEM(w_second.shape, BF),
            pltpu.VMEM(bilinear.shape, F32),
            pltpu.VMEM(w_last.shape, BF),
            *[pltpu.VMEM(s, d) for s, d in shapes],
            pltpu.SemaphoreType.DMA((4,)),
            pltpu.SemaphoreType.DMA((len(shapes),)),
        ],
        compiler_params=params(12),
        name="prepare",
    )(*far(order, w_first, w_second, bilinear, w_last))


def owner_body(placement_hbm, *refs):
    count = 12
    sources, (kept_hbm, moved_hbm, send_hbm) = refs[:count], refs[count : count + 3]
    placement = refs[count + 3]
    loaded = refs[count + 4 : 2 * count + 4]
    kept, moved, send, embeds_ref, product_ref, grad_ref, flat, sems, out_sems = refs[2 * count + 4 :]
    arrived, labels, senet_in, senet_out, kron_high, kron_low, first_turned, second_turned, last, second, back_high, first = loaded
    tables = pltpu.make_async_copy(placement_hbm, placement, sems.at[count])
    tables.start()
    loads = [pltpu.make_async_copy(sources[i], loaded[i], sems.at[i]) for i in range(count)]
    for copy in loads:
        copy.start()

    fields = placement.shape[0]
    total, lanes = arrived.shape
    width = total // fields
    factor = fields ** -0.5
    chunk = kron_high.shape[0]
    per = chunk // width
    chips, rows, _ = kept.shape
    step = min(chunk, rows)
    hidden = second.shape[0]
    mine = lax.axis_index("tab")
    core = mine % 2
    tables.wait()
    loads[0].wait()
    for s in range(fields):
        spot = pl.multiple_of(placement[s] * width, width)
        embeds_ref[pl.ds(spot, width), :] = arrived[s * width : (s + 1) * width, :]

    dense3 = embeds_ref[...].astype(F32).reshape(fields, width, lanes)
    squeeze = jnp.sum(dense3, axis=1) * (1.0 / width)
    for copy in loads[1:6]:
        copy.wait()
    pre_one = dot(senet_in[...], squeeze, NN, PRECISE)
    act_one = pre_one * jax.nn.sigmoid(pre_one)
    weights = jax.nn.sigmoid(dot(senet_out[...], act_one, TN, PRECISE))
    sum_plain = jnp.zeros((width, lanes), F32)
    sum_scaled = jnp.zeros((width, lanes), F32)
    for f in range(fields):
        one = embeds_ref[f * width : (f + 1) * width, :].astype(F32)
        sum_plain = sum_plain + one
        sum_scaled = sum_scaled + one * weights[f : f + 1, :]
    loads[6].wait()
    pre_hidden = jnp.zeros((hidden, lanes), F32)
    for g in range(0, total, chunk):
        block = embeds_ref[g : g + chunk, :]
        product = dot(kron_high[...], block) + dot(kron_low[...], block)
        product_ref[g : g + chunk, :] = product
        product3 = product.reshape(per, width, lanes) * factor
        dense = block.astype(F32).reshape(per, width, lanes)
        scale = weights[g // width : g // width + per][:, None, :]
        plain = (product3 * (sum_plain[None] - dense)).reshape(chunk, lanes).astype(BF)
        scaled = (product3 * scale * (sum_scaled[None] - dense * scale)).reshape(chunk, lanes).astype(BF)
        for start, values in ((g, plain), (total + g, scaled)):
            pre_hidden = pre_hidden + dot(first_turned[:, start : start + chunk], values)
            for piece in range(0, chunk, step):
                owner, spot = divmod(start + piece, rows)
                part = values[piece : piece + step]

                @pl.when(core == owner % 2)
                def _():
                    kept[owner // 2, spot : spot + step, :] = part

                @pl.when(core != owner % 2)
                def _():
                    moved[owner // 2 * rows + spot : owner // 2 * rows + spot + step, :] = part

    leave_kept = pltpu.make_async_copy(kept, kept_hbm, out_sems.at[0])
    leave_kept.start()
    for copy in loads[7:]:
        copy.wait()
    hidden_one = (pre_hidden * jax.nn.sigmoid(pre_hidden)).astype(BF)
    pre_second = dot(second_turned[...], hidden_one)
    hidden_two = (pre_second * jax.nn.sigmoid(pre_second)).astype(BF)
    hidden_wide = hidden_two.astype(F32)
    last_wide = last[...]
    logits = jnp.sum(last_wide * hidden_wide, axis=0, keepdims=True)
    grad_logit = jax.nn.sigmoid(logits) - labels[pl.ds(mine, 1), :].astype(F32)
    d_last = jnp.sum(hidden_wide * grad_logit, axis=1, keepdims=True)
    d_pre_two = (grad_logit * last_wide * silu_slope(pre_second)).astype(BF)
    flat[:hidden, :] = dot(hidden_one, d_pre_two, NT)
    d_pre_one = (dot(second[...], d_pre_two) * silu_slope(pre_hidden)).astype(BF)
    moved[chips * rows :, :] = d_pre_one
    leave_moved = pltpu.make_async_copy(moved, moved_hbm, out_sems.at[1])
    leave_moved.start()

    rest_plain = jnp.zeros((width, lanes), F32)
    rest_scaled = jnp.zeros((width, lanes), F32)
    bil = jnp.zeros((chunk, chunk), F32)
    d_weight_parts = []
    for g in range(0, total, chunk):
        d_plain = dot(first[g : g + chunk, :], d_pre_one).reshape(per, width, lanes)
        d_scaled = dot(first[total + g : total + g + chunk, :], d_pre_one).reshape(per, width, lanes)
        block = embeds_ref[g : g + chunk, :]
        dense = block.astype(F32).reshape(per, width, lanes)
        scale = weights[g // width : g // width + per][:, None, :]
        product = product_ref[g : g + chunk, :].reshape(per, width, lanes) * factor
        others_scaled = d_scaled * product
        d_others_plain = d_plain * product
        d_others_scaled = others_scaled * scale
        rest_plain = rest_plain + jnp.sum(d_others_plain, axis=0)
        rest_scaled = rest_scaled + jnp.sum(d_others_scaled, axis=0)
        away_scaled = sum_scaled[None] - dense * scale
        d_product = (d_plain * (sum_plain[None] - dense) + d_scaled * scale * away_scaled) * factor
        direct = d_product.reshape(chunk, lanes).astype(BF)
        bil = bil + dot(block, direct, NT)
        back = dot(back_high[...], direct).reshape(per, width, lanes)
        grad = back - d_others_plain - d_others_scaled * scale
        grad_ref[g : g + chunk, :] = grad.reshape(chunk, lanes)
        d_weight_parts.append(jnp.sum(others_scaled * away_scaled - dense * d_others_scaled, axis=1))
    d_bil = bil[0:width, 0:width]
    for i in range(1, per):
        d_bil = d_bil + bil[i * width : (i + 1) * width, i * width : (i + 1) * width]
    dense3 = embeds_ref[...].astype(F32).reshape(fields, width, lanes)
    d_weights = jnp.concatenate(d_weight_parts, axis=0) + jnp.sum(dense3 * rest_scaled[None], axis=1)
    d_pre_w = d_weights * weights * (1.0 - weights)
    d_out = dot(act_one, d_pre_w, NT, PRECISE)
    d_act = dot(senet_out[...], d_pre_w, NN, PRECISE) * silu_slope(pre_one)
    d_in = dot(d_act, squeeze, NT, PRECISE)
    d_squeeze = dot(senet_in[...], d_act, TN, PRECISE) * (1.0 / width)
    total_grad = (
        grad_ref[...].reshape(fields, width, lanes)
        + rest_plain[None]
        + weights[:, None, :] * rest_scaled[None]
        + d_squeeze[:, None, :]
    )
    grad_ref[...] = total_grad.reshape(total, lanes)
    tab, depth, _ = send.shape
    slots = fields // tab
    for s in range(fields):
        spot = pl.multiple_of(placement[s] * width, width)
        at = s % slots * width
        send[s // slots, at : at + width, :] = grad_ref[pl.ds(spot, width), :].astype(BF)
    senet = senet_in.shape[0]
    lines = flat.shape[0] // tab
    columns = [d_in, d_out, d_bil] + [d_last[i : i + senet, :] for i in range(0, hidden, senet)]
    used = sum(c.shape[1] for c in columns)
    flat[hidden:, :] = jnp.zeros((flat.shape[0] - hidden, hidden), F32)
    flat[hidden : hidden + senet, :] = jnp.concatenate(columns + [jnp.zeros((senet, hidden - used), F32)], axis=1)
    high = logits.astype(BF).astype(F32)
    base = slots * width
    spare = jnp.zeros((depth - base - hidden // lanes * lines - 2, lanes), F32)
    for t in range(tab):
        band = flat[t * lines : (t + 1) * lines, :]
        pieces = [band[:, i : i + lanes] for i in range(0, hidden, lanes)] + [high, logits - high, spare]
        send[t, base:, :] = jnp.concatenate(pieces, axis=0).astype(BF)
    leave_send = pltpu.make_async_copy(send, send_hbm, out_sems.at[2])
    leave_send.start()
    leave_kept.wait()
    leave_moved.wait()
    leave_send.wait()


def depth_of(base, lines, hidden, lanes):
    return -(-(base + hidden // lanes * lines + 2) // 16) * 16


def owner_pass(placement, arrived, labels, senet_in, senet_out, kron_high, kron_low, first_turned, second_turned, last, w_second, back_high, w_first):
    total, lanes = arrived.shape
    senet, fields = senet_in.shape
    hidden = w_second.shape[0]
    tab = labels.shape[0]
    rows = 2 * total // tab
    lines = -(-(hidden + senet) // tab)
    depth = depth_of(total // tab, lines, hidden, lanes)
    shapes = (((tab // 2, rows, lanes), BF), ((total + hidden, lanes), BF), ((tab, depth, lanes), BF))
    operands = (arrived, labels, senet_in, senet_out, kron_high, kron_low, first_turned, second_turned, last, w_second, back_high, w_first)
    return pl.pallas_call(
        owner_body,
        out_shape=tuple(pltpu.HBM(s, d) for s, d in shapes),
        in_specs=[hspec()] * (1 + len(operands)),
        out_specs=tuple(hspec() for _ in shapes),
        scratch_shapes=[
            pltpu.SMEM((fields,), jnp.int32),
            *[pltpu.VMEM(o.shape, o.dtype) for o in operands],
            *[pltpu.VMEM(s, d) for s, d in shapes],
            pltpu.VMEM((total, lanes), BF),
            pltpu.VMEM((total, lanes), F32),
            pltpu.VMEM((total, lanes), F32),
            pltpu.VMEM((lines * tab, hidden), F32),
            pltpu.SemaphoreType.DMA((len(operands) + 1,)),
            pltpu.SemaphoreType.DMA((3,)),
        ],
        compiler_params=params(24),
        name="owner_pass",
    )(*far(placement), arrived, *far(*operands[1:]))


def first_body(kept_hbm, moved_hbm, came_hbm, *rest):
    kept, moved, came, made, sems, out_sems = rest[-6:]
    outs = rest[:-6]
    chips, rows, _ = kept.shape
    chip = lax.axis_index("tab") // 2
    hidden = moved.shape[0]
    tail = pl.ds(chips * rows, hidden)
    heads = [
        pltpu.make_async_copy(moved_hbm.at[tail], moved, sems.at[0]),
        pltpu.make_async_copy(came_hbm.at[tail], came.at[tail], sems.at[1]),
    ]
    for copy in heads:
        copy.start()
    order = list(range(1, chips)) + [0]
    bodies = {}
    for q in order:
        target = chip ^ q
        part = pl.ds(pl.multiple_of(target * rows, rows), rows)
        bodies[q] = (
            pltpu.make_async_copy(kept_hbm.at[target], kept.at[q], sems.at[2 + 2 * q]),
            pltpu.make_async_copy(came_hbm.at[part], came.at[pl.ds(q * rows, rows)], sems.at[3 + 2 * q]),
        )
        for copy in bodies[q]:
            copy.start()
    for copy in heads:
        copy.wait()
    right = jnp.concatenate([moved[...], came[chips * rows :, :]], axis=1)
    gone = []
    for q in order:
        for copy in bodies[q]:
            copy.wait()
        left = jnp.concatenate([kept[q], came[q * rows : (q + 1) * rows, :]], axis=1)
        made[q] = dot(left, right, NT).astype(BF)
        copy = pltpu.make_async_copy(made.at[q], outs[q], out_sems.at[q])
        copy.start()
        gone.append(copy)
    for copy in gone:
        copy.wait()


def first_grad(kept, moved, came):
    chips, rows, lanes = kept.shape
    hidden = moved.shape[0] - chips * rows
    return pl.pallas_call(
        first_body,
        out_shape=tuple(pltpu.HBM((rows, hidden), BF) for _ in range(chips)),
        in_specs=[hspec()] * 3,
        out_specs=tuple(hspec() for _ in range(chips)),
        scratch_shapes=[
            pltpu.VMEM(kept.shape, BF),
            pltpu.VMEM((hidden, lanes), BF),
            pltpu.VMEM(came.shape, BF),
            pltpu.VMEM((chips, rows, hidden), BF),
            pltpu.SemaphoreType.DMA((2 + 2 * chips,)),
            pltpu.SemaphoreType.DMA((chips,)),
        ],
        compiler_params=params(8),
        name="first_grad",
    )(*far(kept, moved), came)


def tab_body(grads_any, route, summed_out, scores, grads, sem, *, base, line):
    tab, depth, owner = grads.shape
    copy = pltpu.make_async_copy(grads_any.at[:, pl.ds(base, depth), :], grads, sem)
    copy.start()
    wanted = route[pl.ds(lax.axis_index("tab"), 1), :]
    spot = lax.broadcasted_iota(jnp.int32, (owner, owner), 0)
    copy.wait()
    small = grads[0].astype(F32)
    for o in range(1, tab):
        small = small + grads[o].astype(F32)
    summed_out[...] = small.astype(BF)
    found = jnp.zeros((2, owner), F32)
    for o in range(tab):
        found = found + dot(grads[o, line : line + 2, :], (spot + o * owner == wanted).astype(F32).astype(BF))
    scores[...] = found[0:1] + found[1:2]


def tab_sums(grads, route, base, line):
    tab, depth, owner = grads.shape
    return pl.pallas_call(
        functools.partial(tab_body, base=base, line=line),
        out_shape=(
            jax.ShapeDtypeStruct((depth - base, owner), BF),
            jax.ShapeDtypeStruct((1, owner), F32),
        ),
        in_specs=[hspec(), vspec()],
        out_specs=(vspec(), vspec()),
        scratch_shapes=[pltpu.VMEM((tab, depth - base, owner), BF), pltpu.SemaphoreType.DMA(())],
        compiler_params=params(4),
        name="tab_sums",
    )(grads, route)


def slot_body(
    widths_hbm, placement_hbm, pooled, weight_hbm, grads_any, d_pooled, d_proj_hbm,
    widths, placement, rows_in, weight, grads, made, spread, d_proj, sems, in_sems, out_sems,
):
    slots, _, padded = rows_in.shape
    tab, total, owner = grads.shape
    width = total // slots
    first = lax.axis_index("tab") * slots
    pairs = (
        (grads_any.at[:, pl.ds(0, total), :], grads), (weight_hbm, weight), (placement_hbm, placement), (widths_hbm, widths),
    )
    copies = [pltpu.make_async_copy(source, target, sems.at[i]) for i, (source, target) in enumerate(pairs)]
    large = [pltpu.make_async_copy(pooled.at[s], rows_in.at[s], in_sems.at[s]) for s in range(slots)]
    for copy in copies + large:
        copy.start()
    spread[...] = jnp.zeros(spread.shape, BF)
    for copy in copies:
        copy.wait()
    for s in range(slots):
        spread[s * width : (s + 1) * width, s * padded : (s + 1) * padded] = weight[s * width : (s + 1) * width, :]
    gone = []
    for o in range(tab):
        part = slice(o * owner, (o + 1) * owner)
        back = dot(grads[o], spread[...], TN).astype(BF)
        for s in range(slots):
            made[s, part, :] = back[:, s * padded : (s + 1) * padded]
        copy = pltpu.make_async_copy(made.at[:, part, :], d_pooled.at[:, part, :], out_sems.at[o])
        copy.start()
        gone.append(copy)
    lane = lax.broadcasted_iota(jnp.int32, (width, padded), 1)
    for s in range(slots):
        left = jnp.concatenate([grads[o, s * width : (s + 1) * width, :] for o in range(tab)], axis=1)
        keep = lane < widths[placement[first + s]]
        large[s].wait()
        d_proj[s * width : (s + 1) * width, :] = jnp.where(keep, dot(left, rows_in[s]), 0.0).astype(BF)
    copy = pltpu.make_async_copy(d_proj, d_proj_hbm, sems.at[0])
    copy.start()
    gone.append(copy)
    for copy in gone:
        copy.wait()


def slot_grad(widths, placement, pooled, weight, grads):
    slots, _, padded = pooled.shape
    total = weight.shape[0]
    fields = placement.shape[0]
    tab, _, owner = grads.shape
    return pl.pallas_call(
        slot_body,
        out_shape=(pltpu.HBM(pooled.shape, BF), pltpu.HBM((total, padded), BF)),
        in_specs=[hspec()] * 5,
        out_specs=(hspec(), hspec()),
        scratch_shapes=[
            pltpu.SMEM((fields,), jnp.int32),
            pltpu.SMEM((fields,), jnp.int32),
            pltpu.VMEM(pooled.shape, BF),
            pltpu.VMEM(weight.shape, BF),
            pltpu.VMEM((tab, total, owner), BF),
            pltpu.VMEM(pooled.shape, BF),
            pltpu.VMEM((total, slots * padded), BF),
            pltpu.VMEM((total, padded), BF),
            pltpu.SemaphoreType.DMA((4,)),
            pltpu.SemaphoreType.DMA((slots,)),
            pltpu.SemaphoreType.DMA((tab,)),
        ],
        compiler_params=params(14),
        name="slot_grad",
    )(*far(widths, placement, pooled, weight), grads)


def rep_body(*refs):
    parts, small = refs[:-1], refs[-1]
    summed = parts[0][...].astype(F32)
    for part in parts[1:]:
        summed = summed + part[...].astype(F32)
    lines = summed.astype(BF)
    for t in range(small.shape[0]):
        small[t] = lines


def rep_sums(parts, tab):
    return pl.pallas_call(
        rep_body,
        out_shape=jax.ShapeDtypeStruct((tab,) + parts[0].shape, BF),
        in_specs=[vspec()] * len(parts),
        out_specs=vspec(),
        compiler_params=params(4),
        name="rep_sums",
    )(*parts)


def unpack_body(arrived, d_second, d_in, d_out, d_bil, d_last, flat):
    tab, _, lanes = arrived.shape
    hidden = d_second.shape[0]
    lines = flat.shape[0] // tab
    for t in range(tab):
        block = arrived[t].astype(F32)
        for i in range(hidden // lanes):
            flat[t * lines : (t + 1) * lines, i * lanes : (i + 1) * lanes] = block[i * lines : (i + 1) * lines]
    d_second[...] = flat[:hidden, :]
    senet, fields = d_in.shape
    width = d_bil.shape[0]
    band = flat[hidden : hidden + senet, :]
    d_in[...] = band[:, :fields]
    d_out[...] = band[:, fields : 2 * fields]
    d_bil[...] = band[:width, 2 * fields : 2 * fields + width]
    column = 2 * fields + width
    pieces = jnp.concatenate([band[:, column + i : column + i + 1] for i in range(hidden // senet)], axis=0)
    row = lax.broadcasted_iota(jnp.int32, (hidden, hidden), 0)
    across = lax.broadcasted_iota(jnp.int32, (hidden, hidden), 1)
    d_last[...] = jnp.sum(jnp.where(row == across, pieces, 0.0), axis=0, keepdims=True)


def unpack(arrived, hidden, senet, fields, width):
    tab = arrived.shape[0]
    lines = -(-(hidden + senet) // tab)
    shapes = ((hidden, hidden), (senet, fields), (senet, fields), (width, width), (1, hidden))
    return pl.pallas_call(
        unpack_body,
        out_shape=tuple(jax.ShapeDtypeStruct(s, F32) for s in shapes),
        in_specs=[vspec()],
        out_specs=tuple(vspec() for _ in shapes),
        scratch_shapes=[pltpu.VMEM((lines * tab, hidden), F32)],
        compiler_params=params(4),
        name="unpack",
    )(arrived)


def swap(x, axis, size, bit):
    return lax.ppermute(x, axis, [(i, i ^ bit) for i in range(size)])


def shards(pooled, widths, placement, route, labels, proj, senet_in, senet_out, bilinear, w_first, w_second, w_last):
    tab = lax.axis_size("tab")
    rep = lax.axis_size("rep")
    rep_index = lax.axis_index("rep")
    slots, rep_rows, padded = pooled.shape
    fields, senet = senet_in.shape
    width = proj.shape[2]
    owner = rep_rows // tab
    hidden = w_second.shape[0]
    chips = tab // 2

    local, weight = embed_slots(widths, placement, pooled, proj.transpose(0, 2, 1), tab)
    arrived = lax.all_to_all(local, "tab", 0, 0, tiled=True).reshape(fields * width, owner)
    first_turned, second_turned, kron_high, kron_low, back_high, last_column = prepare(
        weight, w_first, w_second, bilinear, w_last.reshape(1, hidden)
    )
    kept, moved, send = owner_pass(
        placement, arrived, labels.reshape(tab, owner), senet_in.T, senet_out, kron_high, kron_low,
        first_turned, second_turned, last_column, w_second, back_high, w_first,
    )
    came = swap(moved, "tab", tab, 1)
    grads = lax.all_to_all(send, "tab", 0, 0, tiled=True)
    parts = first_grad(kept, moved, came)
    rows = parts[0].shape[0]
    sent = [swap(parts[q], "tab", tab, 2 * q) for q in range(1, chips)]

    base = slots * width
    line = hidden // owner * -(-(hidden + senet) // tab)
    small, scores = tab_sums(grads, route.reshape(tab, owner), base, line)
    smalls = [small] + [swap(small, "rep", rep, q) for q in range(1, rep)]
    d_pooled, d_proj = slot_grad(widths, placement, pooled, weight, grads)
    projs = [d_proj] + [swap(d_proj, "rep", rep, q) for q in range(1, rep)]
    proj_sum = sum(p.astype(F32) for p in projs)
    d_proj = proj_sum.reshape(slots, width, padded).transpose(0, 2, 1)
    small = rep_sums(smalls, tab)
    small = lax.all_to_all(small, "tab", 0, 0, tiled=True)
    g_second, g_in, g_out, g_bil, g_last = unpack(small, hidden, senet, fields, width)

    first_sum = parts[0].astype(F32)
    for part in sent:
        first_sum = first_sum + part.astype(F32)
    low_bit = rep_index % 2
    halves = first_sum.astype(BF).reshape(2, rows // 2, hidden)
    mine = lax.dynamic_index_in_dim(halves, low_bit, 0, keepdims=False)
    theirs = lax.dynamic_index_in_dim(halves, 1 - low_bit, 0, keepdims=False)
    theirs = swap(theirs, "rep", rep, 1)
    mine = (mine.astype(F32) + theirs.astype(F32)).astype(BF)
    bit = 2
    while bit < rep:
        theirs = swap(mine, "rep", rep, bit)
        mine = (mine.astype(F32) + theirs.astype(F32)).astype(BF)
        bit *= 2
    back = swap(mine, "rep", rep, 1)
    d_first = jnp.where(
        low_bit == 0, jnp.concatenate([mine, back], axis=0), jnp.concatenate([back, mine], axis=0)
    ).astype(F32)
    return (
        scores, d_pooled, d_proj, g_in.T, g_out, g_bil, d_first, g_second, g_last.reshape(hidden),
    )


def solution(mesh):
    placed = (
        P("tab", "rep", None), P(), P(), P("rep", None), P("rep", None),
        P(), P(), P(), P(), P(), P(), P(),
    )
    return jax.shard_map(
        shards,
        mesh=mesh,
        in_specs=placed,
        out_specs=(P("rep", "tab"), P("tab", "rep", None), P("tab", None, None), P(), P(), P(), P("tab", None), P(), P()),
        check_vma=False,
    )
```

```python
import functools

import jax
import jax.numpy as jnp
from jax import lax
from jax.experimental import pallas as pl
from jax.experimental.pallas import tpu as pltpu
from jax.sharding import PartitionSpec as P


PRECISE = lax.Precision.HIGHEST
BF = jnp.bfloat16
F32 = jnp.float32
VMEM = pltpu.VMEM
NN = (((1,), (0,)), ((), ()))
NT = (((1,), (1,)), ((), ()))
TN = (((0,), (0,)), ((), ()))


def dot(a, b, dims=NN, precision=None):
    return lax.dot_general(a, b, dims, precision=precision, preferred_element_type=F32)


def split(x):
    high = x.astype(BF)
    return high, (x - high.astype(F32)).astype(BF)


def silu_slope(pre_act):
    logistic = jax.nn.sigmoid(pre_act)
    return logistic * (1.0 + pre_act * (1.0 - logistic))


def vspec():
    return pl.BlockSpec(memory_space=VMEM)


def hspec():
    return pl.BlockSpec(memory_space=pltpu.HBM)


def far(*arrays):
    return tuple(pltpu.with_memory_space_constraint(a, pltpu.HBM) for a in arrays)


def params(mebibytes):
    return pltpu.CompilerParams(vmem_limit_bytes=mebibytes << 20)


def embed_body(widths_hbm, placement_hbm, pooled, proj, *refs):
    weight_out, *outs = refs[:-8]
    widths, placement, rows_in, gathered, weights, staged, sems, out_sems = refs[-8:]
    slots, _, padded = rows_in.shape
    width = proj.shape[1]
    tab, _, owner = staged.shape
    mine = lax.axis_index("tab")
    first = mine * slots
    tables = [
        pltpu.make_async_copy(placement_hbm, placement, sems.at[slots]),
        pltpu.make_async_copy(widths_hbm, widths, sems.at[slots + 1]),
    ]
    for copy in tables:
        copy.start()
    whole = pltpu.make_async_copy(proj, gathered, sems.at[slots + 2])
    whole.start()
    large = [pltpu.make_async_copy(pooled.at[s], rows_in.at[s], sems.at[s]) for s in range(slots)]
    for copy in large:
        copy.start()
    for copy in tables:
        copy.wait()
    whole.wait()
    lane = lax.broadcasted_iota(jnp.int32, (width, padded), 1)
    gone = []
    for s in range(slots):
        part = slice(s * width, (s + 1) * width)
        field = placement[first + s]
        weight = jnp.where(lane < widths[field], gathered[field].astype(F32), 0.0).astype(BF)
        weights[part, :] = weight
        large[s].wait()
        embeds = dot(weight, rows_in[s], NT).astype(BF)
        for o in range(tab):
            staged[o, part, :] = embeds[:, o * owner : (o + 1) * owner]
    pairs = [(staged.at[mine ^ q], outs[q]) for q in range(1, tab)] + [(staged.at[mine], outs[0]), (weights, weight_out)]
    for i, (source, target) in enumerate(pairs):
        copy = pltpu.make_async_copy(source, target, out_sems.at[i])
        copy.start()
        gone.append(copy)
    for copy in gone:
        copy.wait()


def embed_slots(widths, placement, pooled, proj, tab):
    slots, rows, padded = pooled.shape
    width = proj.shape[1]
    fields = placement.shape[0]
    return pl.pallas_call(
        embed_body,
        out_shape=(pltpu.HBM((slots * width, padded), BF),) + (pltpu.HBM((slots * width, rows // tab), BF),) * tab,
        in_specs=[hspec()] * 4,
        out_specs=(hspec(),) * (1 + tab),
        scratch_shapes=[
            pltpu.SMEM((fields,), jnp.int32),
            pltpu.SMEM((fields,), jnp.int32),
            pltpu.VMEM((slots, rows, padded), BF),
            pltpu.VMEM(proj.shape, BF),
            pltpu.VMEM((slots * width, padded), BF),
            pltpu.VMEM((tab, slots * width, rows // tab), BF),
            pltpu.SemaphoreType.DMA((slots + 3,)),
            pltpu.SemaphoreType.DMA((tab + 1,)),
        ],
        compiler_params=params(12),
        name="embed_slots",
    )(*far(widths, placement, pooled, proj))


def prepare_body(order, first_hbm, second_hbm, bilinear_hbm, last_hbm, *rest):
    outs, (first, second, bilinear, last), made, sems, out_sems = rest[:6], rest[6:10], rest[10:16], rest[16], rest[17]
    first_turned, second_turned, kron_high, kron_low, back_high, last_column = made
    copies = [
        pltpu.make_async_copy(source, target, sems.at[i])
        for i, (source, target) in enumerate(
            ((bilinear_hbm, bilinear), (last_hbm, last), (second_hbm, second), (first_hbm, first))
        )
    ]
    for copy in copies:
        copy.start()
    leaving = [pltpu.make_async_copy(made[i], outs[i], out_sems.at[i]) for i in range(len(outs))]
    width = bilinear.shape[0]
    side = kron_high.shape[0]
    copies[0].wait()
    tiled = jnp.concatenate([bilinear[...]] * (side // width), axis=1)
    tiled = jnp.concatenate([tiled] * (side // width), axis=0)
    row = lax.broadcasted_iota(jnp.int32, (side, side), 0) // width
    column = lax.broadcasted_iota(jnp.int32, (side, side), 1) // width
    kron = jnp.where(row == column, tiled, 0.0)
    back_high[...] = kron.astype(BF)
    kron_high[...], kron_low[...] = split(kron.T)
    hidden = last.shape[1]
    row = lax.broadcasted_iota(jnp.int32, (hidden, hidden), 0)
    column = lax.broadcasted_iota(jnp.int32, (hidden, hidden), 1)
    copies[1].wait()
    last_column[...] = jnp.sum(jnp.where(row == column, last[...].astype(F32), 0.0), axis=1, keepdims=True)
    copies[2].wait()
    second_turned[...] = second[...].T
    for copy in leaving[1:]:
        copy.start()
    copies[3].wait()
    step = min(512, first.shape[0])
    for g in range(0, first.shape[0], step):
        first_turned[:, g : g + step] = first[g : g + step, :].T
    leaving[0].start()
    for copy in leaving:
        copy.wait()


def prepare(order, w_first, w_second, bilinear, w_last):
    total, hidden = w_first.shape
    side = min(256, total)
    shapes = (
        ((hidden, total), BF), ((hidden, hidden), BF), ((side, side), BF), ((side, side), BF), ((side, side), BF),
        ((hidden, 1), F32),
    )
    return pl.pallas_call(
        prepare_body,
        out_shape=tuple(pltpu.HBM(s, d) for s, d in shapes),
        in_specs=[hspec()] * 5,
        out_specs=tuple(hspec() for _ in shapes),
        scratch_shapes=[
            pltpu.VMEM(w_first.shape, BF),
            pltpu.VMEM(w_second.shape, BF),
            pltpu.VMEM(bilinear.shape, F32),
            pltpu.VMEM(w_last.shape, BF),
            *[pltpu.VMEM(s, d) for s, d in shapes],
            pltpu.SemaphoreType.DMA((4,)),
            pltpu.SemaphoreType.DMA((len(shapes),)),
        ],
        compiler_params=params(12),
        name="prepare",
    )(*far(order, w_first, w_second, bilinear, w_last))


def owner_body(placement_hbm, *refs):
    *refs, joined, send, embeds_ref, product_ref, grad_ref, gate_ref, flat, sems, out_sems = refs
    count = 11
    loaded = refs[-count:]
    placement, arrived = refs[-count - 2 : -count]
    kept_out, moved_out, send_hbm = refs[-count - 5 : -count - 2]
    sources = refs[: -count - 5]
    tab = arrived.shape[0]
    labels, senet_in, senet_out, kron_high, kron_low, first_turned, second_turned, last, second, back_high, first = loaded
    tables = pltpu.make_async_copy(placement_hbm, placement, sems.at[count])
    tables.start()
    pieces = [pltpu.make_async_copy(sources[q], arrived.at[q], sems.at[count + 1 + q]) for q in range(tab)]
    for copy in pieces:
        copy.start()
    loads = [pltpu.make_async_copy(sources[tab + i], loaded[i], sems.at[i]) for i in range(count)]
    for copy in loads[:6]:
        copy.start()

    fields = placement.shape[0]
    lanes = arrived.shape[2]
    total = tab * arrived.shape[1]
    width = total // fields
    factor = fields ** -0.5
    chunk = kron_high.shape[0]
    per = chunk // width
    hidden = second.shape[0]
    depth = send.shape[1]
    slots = fields // tab
    rows = 2 * total // tab
    step = min(chunk, rows)
    mine = lax.axis_index("tab")
    core = mine % 2
    tables.wait()
    for q in range(tab):
        pieces[q].wait()
        for i in range(slots):
            spot = pl.multiple_of(placement[(mine ^ q) * slots + i] * width, width)
            embeds_ref[pl.ds(spot, width), :] = arrived[q, i * width : (i + 1) * width, :]

    dense3 = embeds_ref[...].astype(F32).reshape(fields, width, lanes)
    squeeze = jnp.sum(dense3, axis=1) * (1.0 / width)
    for copy in loads[:5]:
        copy.wait()
    for copy in loads[6:]:
        copy.start()
    pre_one = dot(senet_in[...], squeeze, NN, PRECISE)
    act_one = pre_one * jax.nn.sigmoid(pre_one)
    weights = jax.nn.sigmoid(dot(senet_out[...], act_one, TN, PRECISE))
    sum_plain = jnp.zeros((width, lanes), F32)
    sum_scaled = jnp.zeros((width, lanes), F32)
    for f in range(fields):
        one = embeds_ref[f * width : (f + 1) * width, :].astype(F32)
        sum_plain = sum_plain + one
        sum_scaled = sum_scaled + one * weights[f : f + 1, :]
    for g in range(0, total, chunk):
        block = embeds_ref[g : g + chunk, :]
        product = dot(kron_high[...], block) + dot(kron_low[...], block)
        product_ref[g : g + chunk, :] = product
        product3 = product.reshape(per, width, lanes) * factor
        dense = block.astype(F32).reshape(per, width, lanes)
        scale = weights[g // width : g // width + per][:, None, :]
        plain = (product3 * (sum_plain[None] - dense)).reshape(chunk, lanes).astype(BF)
        scaled = (product3 * scale * (sum_scaled[None] - dense * scale)).reshape(chunk, lanes).astype(BF)
        for start, values in ((g, plain), (total + g, scaled)):
            for piece in range(0, chunk, step):
                owner, spot = divmod(start + piece, rows)
                at = owner // 2 * rows + spot
                joined[(owner % 2) ^ core, at : at + step, :] = values[piece : piece + step]
    blocks = [joined[(o % 2) ^ core, o // 2 * rows : (o // 2 + 1) * rows, :] for o in range(tab)]
    loads[5].wait()
    pre_hidden = dot(first_turned[...], jnp.concatenate(blocks, axis=0))
    for copy in loads[6:]:
        copy.wait()
    hidden_one = (pre_hidden * jax.nn.sigmoid(pre_hidden)).astype(BF)
    pre_second = dot(second_turned[...], hidden_one)
    hidden_two = (pre_second * jax.nn.sigmoid(pre_second)).astype(BF)
    hidden_wide = hidden_two.astype(F32)
    last_wide = last[...]
    logits = jnp.sum(last_wide * hidden_wide, axis=0, keepdims=True)
    grad_logit = jax.nn.sigmoid(logits) - labels[pl.ds(mine, 1), :].astype(F32)
    d_last = jnp.sum(hidden_wide * grad_logit, axis=1, keepdims=True)
    d_pre_two = (grad_logit * last_wide * silu_slope(pre_second)).astype(BF)
    flat[:hidden, :] = dot(hidden_one, d_pre_two, NT)
    d_pre_one = (dot(second[...], d_pre_two) * silu_slope(pre_hidden)).astype(BF)
    joined[0, total:, :] = d_pre_one
    joined[1, total:, :] = d_pre_one
    leave_moved = pltpu.make_async_copy(joined.at[1], moved_out, out_sems.at[1])
    leave_moved.start()
    leave_kept = pltpu.make_async_copy(joined.at[0], kept_out, out_sems.at[0])
    leave_kept.start()

    rest_plain = jnp.zeros((width, lanes), F32)
    rest_scaled = jnp.zeros((width, lanes), F32)
    bil = jnp.zeros((chunk, chunk), F32)
    d_weight_parts = []
    for g in range(0, total, chunk):
        d_plain = dot(first[g : g + chunk, :], d_pre_one).reshape(per, width, lanes)
        d_scaled = dot(first[total + g : total + g + chunk, :], d_pre_one).reshape(per, width, lanes)
        block = embeds_ref[g : g + chunk, :]
        dense = block.astype(F32).reshape(per, width, lanes)
        scale = weights[g // width : g // width + per][:, None, :]
        product = product_ref[g : g + chunk, :].reshape(per, width, lanes) * factor
        others_scaled = d_scaled * product
        d_others_plain = d_plain * product
        d_others_scaled = others_scaled * scale
        rest_plain = rest_plain + jnp.sum(d_others_plain, axis=0)
        rest_scaled = rest_scaled + jnp.sum(d_others_scaled, axis=0)
        away_scaled = sum_scaled[None] - dense * scale
        d_product = (d_plain * (sum_plain[None] - dense) + d_scaled * scale * away_scaled) * factor
        direct = d_product.reshape(chunk, lanes).astype(BF)
        bil = bil + dot(block, direct, NT)
        back = dot(back_high[...], direct).reshape(per, width, lanes)
        grad = back - d_others_plain - d_others_scaled * scale
        grad_ref[g : g + chunk, :] = grad.reshape(chunk, lanes)
        d_weight_parts.append(jnp.sum(others_scaled * away_scaled - dense * d_others_scaled, axis=1))
    d_bil = bil[0:width, 0:width]
    for i in range(1, per):
        d_bil = d_bil + bil[i * width : (i + 1) * width, i * width : (i + 1) * width]
    dense3 = embeds_ref[...].astype(F32).reshape(fields, width, lanes)
    d_weights = jnp.concatenate(d_weight_parts, axis=0) + jnp.sum(dense3 * rest_scaled[None], axis=1)
    d_pre_w = d_weights * weights * (1.0 - weights)
    d_out = dot(act_one, d_pre_w, NT, PRECISE)
    d_act = dot(senet_out[...], d_pre_w, NN, PRECISE) * silu_slope(pre_one)
    d_in = dot(d_act, squeeze, NT, PRECISE)
    d_squeeze = dot(senet_in[...], d_act, TN, PRECISE) * (1.0 / width)
    gate_ref[0] = weights
    gate_ref[1] = d_squeeze
    for s in range(fields):
        spot = pl.multiple_of(placement[s] * width, width)
        at = s % slots * width
        grad = grad_ref[pl.ds(spot, width), :] + rest_plain
        grad = grad + (gate_ref[0, pl.ds(placement[s], 1), :] * rest_scaled + gate_ref[1, pl.ds(placement[s], 1), :])
        send[s // slots, at : at + width, :] = grad.astype(BF)
    senet = senet_in.shape[0]
    lines = flat.shape[0] // tab
    columns = [d_in, d_out, d_bil] + [d_last[i : i + senet, :] for i in range(0, hidden, senet)]
    used = sum(c.shape[1] for c in columns)
    flat[hidden:, :] = jnp.zeros((flat.shape[0] - hidden, hidden), F32)
    flat[hidden : hidden + senet, :] = jnp.concatenate(columns + [jnp.zeros((senet, hidden - used), F32)], axis=1)
    high = logits.astype(BF).astype(F32)
    base = slots * width
    spare = jnp.zeros((depth - base - hidden // lanes * lines - 2, lanes), F32)
    for t in range(tab):
        band = flat[t * lines : (t + 1) * lines, :]
        pieces = [band[:, i : i + lanes] for i in range(0, hidden, lanes)] + [high, logits - high, spare]
        send[t, base:, :] = jnp.concatenate(pieces, axis=0).astype(BF)
    leave_send = pltpu.make_async_copy(send, send_hbm, out_sems.at[2])
    leave_send.start()
    leave_kept.wait()
    leave_moved.wait()
    leave_send.wait()


def depth_of(base, lines, hidden, lanes):
    return -(-(base + hidden // lanes * lines + 2) // 16) * 16


def owner_pass(placement, arrived, labels, senet_in, senet_out, kron_high, kron_low, first_turned, second_turned, last, w_second, back_high, w_first):
    tab = len(arrived)
    total, lanes = tab * arrived[0].shape[0], arrived[0].shape[1]
    senet, fields = senet_in.shape
    hidden = w_second.shape[0]
    lines = -(-(hidden + senet) // tab)
    depth = depth_of(total // tab, lines, hidden, lanes)
    pair = jax.ShapeDtypeStruct((total + hidden, lanes), BF)
    operands = (labels, senet_in, senet_out, kron_high, kron_low, first_turned, second_turned, last, w_second, back_high, w_first)
    return pl.pallas_call(
        owner_body,
        out_shape=(pair, pair, pltpu.HBM((tab, depth, lanes), BF)),
        in_specs=[hspec()] * (1 + tab + len(operands)),
        out_specs=(vspec(), vspec(), hspec()),
        scratch_shapes=[
            pltpu.SMEM((fields,), jnp.int32),
            pltpu.VMEM((tab, total // tab, lanes), BF),
            *[pltpu.VMEM(o.shape, o.dtype) for o in operands],
            pltpu.VMEM((2, total + hidden, lanes), BF),
            pltpu.VMEM((tab, depth, lanes), BF),
            pltpu.VMEM((total, lanes), BF),
            pltpu.VMEM((total, lanes), F32),
            pltpu.VMEM((total, lanes), F32),
            pltpu.VMEM((2, fields, lanes), F32),
            pltpu.VMEM((lines * tab, hidden), F32),
            pltpu.SemaphoreType.DMA((len(operands) + 1 + tab,)),
            pltpu.SemaphoreType.DMA((3,)),
        ],
        compiler_params=params(24),
        name="owner_pass",
    )(*far(placement), *arrived, *far(*operands))


def first_body(kept, came, *outs):
    chips = len(outs)
    rows, _ = outs[0].shape
    chip = lax.axis_index("tab") // 2
    right = jnp.concatenate([kept[chips * rows :, :], came[chips * rows :, :]], axis=1)
    for q in range(chips):
        part = pl.ds(pl.multiple_of((chip ^ q) * rows, rows), rows)
        left = jnp.concatenate([kept[part, :], came[part, :]], axis=1)
        outs[q][...] = dot(left, right, NT).astype(BF)


def first_grad(kept, came, chips, hidden):
    rows = (kept.shape[0] - hidden) // chips
    return pl.pallas_call(
        first_body,
        out_shape=tuple(jax.ShapeDtypeStruct((rows, hidden), BF) for _ in range(chips)),
        in_specs=[vspec()] * 2,
        out_specs=tuple(vspec() for _ in range(chips)),
        compiler_params=params(8),
        name="first_grad",
    )(kept, came)


def proj_body(
    widths_hbm, placement_hbm, pooled, grads, route_hbm, summed_out, scores,
    widths, placement, rows_in, route, sems, in_sems, *, line,
):
    slots, _, padded = rows_in.shape
    tab, _, owner = grads.shape
    mine = lax.axis_index("tab")
    first = mine * slots
    pairs = ((placement_hbm, placement), (widths_hbm, widths), (route_hbm, route))
    copies = [pltpu.make_async_copy(source, target, sems.at[i]) for i, (source, target) in enumerate(pairs)]
    large = [pltpu.make_async_copy(pooled.at[s], rows_in.at[s], in_sems.at[s]) for s in range(slots)]
    for copy in copies + large:
        copy.start()
    total = line[0]
    width = total // slots
    small = grads[0, total:, :].astype(F32)
    for o in range(1, tab):
        small = small + grads[o, total:, :].astype(F32)
    summed_out[total:, :] = small.astype(BF)
    for copy in copies:
        copy.wait()
    wanted = route[pl.ds(mine, 1), :]
    spot = lax.broadcasted_iota(jnp.int32, (owner, owner), 0)
    found = jnp.zeros((2, owner), F32)
    for o in range(tab):
        found = found + dot(grads[o, line[1] : line[1] + 2, :], (spot + o * owner == wanted).astype(F32).astype(BF))
    scores[...] = found[0:1] + found[1:2]
    lane = lax.broadcasted_iota(jnp.int32, (width, padded), 1)
    for s in range(slots):
        left = jnp.concatenate([grads[o, s * width : (s + 1) * width, :] for o in range(tab)], axis=1)
        keep = lane < widths[placement[first + s]]
        large[s].wait()
        summed_out[s * width : (s + 1) * width, :] = jnp.where(keep, dot(left, rows_in[s]), 0.0).astype(BF)


def proj_grad(widths, placement, pooled, grads, route, total, line):
    slots, _, padded = pooled.shape
    fields = placement.shape[0]
    _, depth, owner = grads.shape
    return pl.pallas_call(
        functools.partial(proj_body, line=(total, line)),
        out_shape=(jax.ShapeDtypeStruct((depth, padded), BF), jax.ShapeDtypeStruct((1, owner), F32)),
        in_specs=[hspec(), hspec(), hspec(), vspec(), hspec()],
        out_specs=(vspec(), vspec()),
        scratch_shapes=[
            pltpu.SMEM((fields,), jnp.int32),
            pltpu.SMEM((fields,), jnp.int32),
            pltpu.VMEM(pooled.shape, BF),
            pltpu.VMEM(route.shape, jnp.int32),
            pltpu.SemaphoreType.DMA((3,)),
            pltpu.SemaphoreType.DMA((slots,)),
        ],
        compiler_params=params(8),
        name="proj_grad",
    )(*far(widths, placement, pooled), grads, *far(route))


def pooled_body(weight_hbm, grads_any, d_pooled, weight, grads, made, spread, sems, out_sems):
    slots, _, padded = made.shape
    tab, total, owner = grads.shape
    width = total // slots
    copies = [
        pltpu.make_async_copy(weight_hbm, weight, sems.at[0]),
        pltpu.make_async_copy(grads_any.at[:, pl.ds(0, total), :], grads, sems.at[1]),
    ]
    for copy in copies:
        copy.start()
    spread[...] = jnp.zeros(spread.shape, BF)
    copies[0].wait()
    for s in range(slots):
        spread[s * width : (s + 1) * width, s * padded : (s + 1) * padded] = weight[s * width : (s + 1) * width, :]
    copies[1].wait()
    gone = []
    for o in range(tab):
        part = slice(o * owner, (o + 1) * owner)
        back = dot(grads[o], spread[...], TN).astype(BF)
        for s in range(slots):
            made[s, part, :] = back[:, s * padded : (s + 1) * padded]
        copy = pltpu.make_async_copy(made.at[:, part, :], d_pooled.at[:, part, :], out_sems.at[o])
        copy.start()
        gone.append(copy)
    for copy in gone:
        copy.wait()


def pooled_grad(pooled, weight, grads):
    slots, _, padded = pooled.shape
    total = weight.shape[0]
    tab, _, owner = grads.shape
    return pl.pallas_call(
        pooled_body,
        out_shape=pltpu.HBM(pooled.shape, BF),
        in_specs=[hspec()] * 2,
        out_specs=hspec(),
        scratch_shapes=[
            pltpu.VMEM(weight.shape, BF),
            pltpu.VMEM((tab, total, owner), BF),
            pltpu.VMEM(pooled.shape, BF),
            pltpu.VMEM((total, slots * padded), BF),
            pltpu.SemaphoreType.DMA((2,)),
            pltpu.SemaphoreType.DMA((tab,)),
        ],
        compiler_params=params(8),
        name="pooled_grad",
    )(*far(weight), grads)


def rep_body(*refs):
    parts, (d_proj, small) = refs[:-2], refs[-2:]
    total = d_proj.shape[0]
    summed = parts[0][...].astype(F32)
    for part in parts[1:]:
        summed = summed + part[...].astype(F32)
    d_proj[...] = summed[:total]
    small[...] = summed[total:].astype(BF)


def rep_sums(parts, total):
    depth, lanes = parts[0].shape
    return pl.pallas_call(
        rep_body,
        out_shape=(
            jax.ShapeDtypeStruct((total, lanes), F32),
            jax.ShapeDtypeStruct((depth - total, lanes), BF),
        ),
        in_specs=[vspec()] * len(parts),
        out_specs=(vspec(), vspec()),
        compiler_params=params(4),
        name="rep_sums",
    )(*parts)


def unpack_body(near, across, d_second, d_in, d_out, d_bil, d_last, arrived, flat):
    tab, _, lanes = arrived.shape
    mine = lax.axis_index("tab")
    for q in range(tab // 2):
        arrived[mine ^ (2 * q)] = near[q]
        arrived[mine ^ (2 * q + 1)] = across[q]
    hidden = d_second.shape[0]
    lines = flat.shape[0] // tab
    for t in range(tab):
        block = arrived[t].astype(F32)
        for i in range(hidden // lanes):
            flat[t * lines : (t + 1) * lines, i * lanes : (i + 1) * lanes] = block[i * lines : (i + 1) * lines]
    d_second[...] = flat[:hidden, :]
    senet, fields = d_in.shape
    width = d_bil.shape[0]
    band = flat[hidden : hidden + senet, :]
    d_in[...] = band[:, :fields]
    d_out[...] = band[:, fields : 2 * fields]
    d_bil[...] = band[:width, 2 * fields : 2 * fields + width]
    column = 2 * fields + width
    pieces = jnp.concatenate([band[:, column + i : column + i + 1] for i in range(hidden // senet)], axis=0)
    row = lax.broadcasted_iota(jnp.int32, (hidden, hidden), 0)
    across = lax.broadcasted_iota(jnp.int32, (hidden, hidden), 1)
    d_last[...] = jnp.sum(jnp.where(row == across, pieces, 0.0), axis=0, keepdims=True)


def unpack(near, across, hidden, senet, fields, width):
    tab = 2 * near.shape[0]
    lines = -(-(hidden + senet) // tab)
    shapes = ((hidden, hidden), (senet, fields), (senet, fields), (width, width), (1, hidden))
    return pl.pallas_call(
        unpack_body,
        out_shape=tuple(jax.ShapeDtypeStruct(s, F32) for s in shapes),
        in_specs=[vspec()] * 2,
        out_specs=tuple(vspec() for _ in shapes),
        scratch_shapes=[pltpu.VMEM((tab,) + near.shape[1:], BF), pltpu.VMEM((lines * tab, hidden), F32)],
        compiler_params=params(4),
        name="unpack",
    )(near, across)


def embeds_order(tab):
    return range(1, tab)


def swap(x, axis, size, bit):
    return lax.ppermute(x, axis, [(i, i ^ bit) for i in range(size)])


def shards(pooled, widths, placement, route, labels, proj, senet_in, senet_out, bilinear, w_first, w_second, w_last):
    tab = lax.axis_size("tab")
    rep = lax.axis_size("rep")
    rep_index = lax.axis_index("rep")
    slots, rep_rows, padded = pooled.shape
    fields, senet = senet_in.shape
    width = proj.shape[2]
    owner = rep_rows // tab
    hidden = w_second.shape[0]
    chips = tab // 2

    weight, *local = embed_slots(widths, placement, pooled, proj.transpose(0, 2, 1), tab)
    arrived = [local[0]] + [swap(local[q], "tab", tab, q) for q in embeds_order(tab)]
    first_turned, second_turned, kron_high, kron_low, back_high, last_column = prepare(
        weight, w_first, w_second, bilinear, w_last.reshape(1, hidden)
    )
    kept, moved, send = owner_pass(
        placement, arrived, labels.reshape(tab, owner), senet_in.T, senet_out, kron_high, kron_low,
        first_turned, second_turned, last_column, w_second, back_high, w_first,
    )
    came = swap(moved, "tab", tab, 1)
    grads = lax.all_to_all(send, "tab", 0, 0, tiled=True)
    parts = first_grad(kept, came, chips, hidden)
    rows = parts[0].shape[0]
    sent = [swap(parts[q], "tab", tab, 2 * q) for q in range(1, chips)]

    base = slots * width
    line = base + hidden // owner * -(-(hidden + senet) // tab)
    summed, scores = proj_grad(widths, placement, pooled, grads, route.reshape(tab, owner), base, line)
    sums = [summed]
    bit = 1
    while bit < rep:
        if len(sums) > 1:
            sums = [sum(part.astype(F32) for part in sums).astype(BF)]
        sums.append(swap(sums[0], "rep", rep, bit))
        bit *= 2
    d_pooled = pooled_grad(pooled, weight, grads)
    d_proj, small = rep_sums(sums, base)
    d_proj = d_proj.reshape(slots, width, padded).transpose(0, 2, 1)
    near = jnp.stack([small] + [swap(small, "tab", tab, 2 * q) for q in range(1, chips)])
    across = swap(near, "tab", tab, 1)
    g_second, g_in, g_out, g_bil, g_last = unpack(near, across, hidden, senet, fields, width)

    first_sum = parts[0].astype(F32)
    for part in sent:
        first_sum = first_sum + part.astype(F32)
    low_bit = rep_index % 2
    halves = first_sum.astype(BF).reshape(2, rows // 2, hidden)
    mine = lax.dynamic_index_in_dim(halves, low_bit, 0, keepdims=False)
    theirs = lax.dynamic_index_in_dim(halves, 1 - low_bit, 0, keepdims=False)
    theirs = swap(theirs, "rep", rep, 1)
    mine = (mine.astype(F32) + theirs.astype(F32)).astype(BF)
    bit = 2
    while bit < rep:
        theirs = swap(mine, "rep", rep, bit)
        mine = (mine.astype(F32) + theirs.astype(F32)).astype(BF)
        bit *= 2
    back = swap(mine, "rep", rep, 1)
    d_first = jnp.where(
        low_bit == 0, jnp.concatenate([mine, back], axis=0), jnp.concatenate([back, mine], axis=0)
    ).astype(F32)
    return (
        scores, d_pooled, d_proj, g_in.T, g_out, g_bil, d_first, g_second, g_last.reshape(hidden),
    )


def solution(mesh):
    placed = (
        P("tab", "rep", None), P(), P(), P("rep", None), P("rep", None),
        P(), P(), P(), P(), P(), P(), P(),
    )
    return jax.shard_map(
        shards,
        mesh=mesh,
        in_specs=placed,
        out_specs=(P("rep", "tab"), P("tab", "rep", None), P("tab", None, None), P(), P(), P(), P("tab", None), P(), P()),
        check_vma=False,
    )
```

```python
import functools

import jax
import jax.numpy as jnp
from jax import lax
from jax.experimental import pallas as pl
from jax.experimental.pallas import tpu as pltpu
from jax.sharding import PartitionSpec as P


PRECISE = lax.Precision.HIGHEST
BF = jnp.bfloat16
F32 = jnp.float32
VMEM = pltpu.VMEM
NN = (((1,), (0,)), ((), ()))
NT = (((1,), (1,)), ((), ()))
TN = (((0,), (0,)), ((), ()))


def dot(a, b, dims=NN, precision=None):
    return lax.dot_general(a, b, dims, precision=precision, preferred_element_type=F32)


def split(x):
    high = x.astype(BF)
    return high, (x - high.astype(F32)).astype(BF)


def silu_slope(pre_act):
    logistic = jax.nn.sigmoid(pre_act)
    return logistic * (1.0 + pre_act * (1.0 - logistic))


def vspec():
    return pl.BlockSpec(memory_space=VMEM)


def hspec():
    return pl.BlockSpec(memory_space=pltpu.HBM)


def far(*arrays):
    return tuple(pltpu.with_memory_space_constraint(a, pltpu.HBM) for a in arrays)


def params(mebibytes):
    return pltpu.CompilerParams(vmem_limit_bytes=mebibytes << 20)


def embed_body(widths_hbm, placement_hbm, pooled, proj, *refs):
    weight_out, *outs = refs[:-8]
    widths, placement, rows_in, gathered, weights, staged, sems, out_sems = refs[-8:]
    slots, _, padded = rows_in.shape
    width = proj.shape[1]
    tab, _, owner = staged.shape
    mine = lax.axis_index("tab")
    first = mine * slots
    tables = [
        pltpu.make_async_copy(placement_hbm, placement, sems.at[slots]),
        pltpu.make_async_copy(widths_hbm, widths, sems.at[slots + 1]),
    ]
    for copy in tables:
        copy.start()
    whole = pltpu.make_async_copy(proj, gathered, sems.at[slots + 2])
    whole.start()
    large = [pltpu.make_async_copy(pooled.at[s], rows_in.at[s], sems.at[s]) for s in range(slots)]
    for copy in large:
        copy.start()
    for copy in tables:
        copy.wait()
    whole.wait()
    lane = lax.broadcasted_iota(jnp.int32, (width, padded), 1)
    gone = []
    for s in range(slots):
        part = slice(s * width, (s + 1) * width)
        field = placement[first + s]
        weight = jnp.where(lane < widths[field], gathered[field].astype(F32), 0.0).astype(BF)
        weights[part, :] = weight
        large[s].wait()
        embeds = dot(weight, rows_in[s], NT).astype(BF)
        for o in range(tab):
            staged[o, part, :] = embeds[:, o * owner : (o + 1) * owner]
    pairs = [(staged.at[mine ^ q], outs[q]) for q in range(1, tab)] + [(staged.at[mine], outs[0]), (weights, weight_out)]
    for i, (source, target) in enumerate(pairs):
        copy = pltpu.make_async_copy(source, target, out_sems.at[i])
        copy.start()
        gone.append(copy)
    for copy in gone:
        copy.wait()


def embed_slots(widths, placement, pooled, proj, tab):
    slots, rows, padded = pooled.shape
    width = proj.shape[1]
    fields = placement.shape[0]
    return pl.pallas_call(
        embed_body,
        out_shape=(pltpu.HBM((slots * width, padded), BF),) + (pltpu.HBM((slots * width, rows // tab), BF),) * tab,
        in_specs=[hspec()] * 4,
        out_specs=(hspec(),) * (1 + tab),
        scratch_shapes=[
            pltpu.SMEM((fields,), jnp.int32),
            pltpu.SMEM((fields,), jnp.int32),
            pltpu.VMEM((slots, rows, padded), BF),
            pltpu.VMEM(proj.shape, BF),
            pltpu.VMEM((slots * width, padded), BF),
            pltpu.VMEM((tab, slots * width, rows // tab), BF),
            pltpu.SemaphoreType.DMA((slots + 3,)),
            pltpu.SemaphoreType.DMA((tab + 1,)),
        ],
        compiler_params=params(12),
        name="embed_slots",
    )(*far(widths, placement, pooled, proj))


def prepare_body(order, first_hbm, second_hbm, bilinear_hbm, last_hbm, *rest):
    outs, (first, second, bilinear, last), made, sems, out_sems = rest[:6], rest[6:10], rest[10:16], rest[16], rest[17]
    first_turned, second_turned, kron_high, kron_low, back_high, last_column = made
    copies = [
        pltpu.make_async_copy(source, target, sems.at[i])
        for i, (source, target) in enumerate(
            ((bilinear_hbm, bilinear), (last_hbm, last), (second_hbm, second), (first_hbm, first))
        )
    ]
    for copy in copies:
        copy.start()
    leaving = [pltpu.make_async_copy(made[i], outs[i], out_sems.at[i]) for i in range(len(outs))]
    width = bilinear.shape[0]
    side = kron_high.shape[0]
    copies[0].wait()
    tiled = jnp.concatenate([bilinear[...]] * (side // width), axis=1)
    tiled = jnp.concatenate([tiled] * (side // width), axis=0)
    row = lax.broadcasted_iota(jnp.int32, (side, side), 0) // width
    column = lax.broadcasted_iota(jnp.int32, (side, side), 1) // width
    kron = jnp.where(row == column, tiled, 0.0)
    back_high[...] = kron.astype(BF)
    kron_high[...], kron_low[...] = split(kron.T)
    hidden = last.shape[1]
    row = lax.broadcasted_iota(jnp.int32, (hidden, hidden), 0)
    column = lax.broadcasted_iota(jnp.int32, (hidden, hidden), 1)
    copies[1].wait()
    last_column[...] = jnp.sum(jnp.where(row == column, last[...].astype(F32), 0.0), axis=1, keepdims=True)
    copies[2].wait()
    second_turned[...] = second[...].T
    for copy in leaving[1:]:
        copy.start()
    copies[3].wait()
    step = min(512, first.shape[0])
    for g in range(0, first.shape[0], step):
        first_turned[:, g : g + step] = first[g : g + step, :].T
    leaving[0].start()
    for copy in leaving:
        copy.wait()


def prepare(order, w_first, w_second, bilinear, w_last):
    total, hidden = w_first.shape
    side = min(256, total)
    shapes = (
        ((hidden, total), BF), ((hidden, hidden), BF), ((side, side), BF), ((side, side), BF), ((side, side), BF),
        ((hidden, 1), F32),
    )
    return pl.pallas_call(
        prepare_body,
        out_shape=tuple(pltpu.HBM(s, d) for s, d in shapes),
        in_specs=[hspec()] * 5,
        out_specs=tuple(hspec() for _ in shapes),
        scratch_shapes=[
            pltpu.VMEM(w_first.shape, BF),
            pltpu.VMEM(w_second.shape, BF),
            pltpu.VMEM(bilinear.shape, F32),
            pltpu.VMEM(w_last.shape, BF),
            *[pltpu.VMEM(s, d) for s, d in shapes],
            pltpu.SemaphoreType.DMA((4,)),
            pltpu.SemaphoreType.DMA((len(shapes),)),
        ],
        compiler_params=params(12),
        name="prepare",
    )(*far(order, w_first, w_second, bilinear, w_last))


def owner_body(placement_hbm, *refs):
    *refs, joined, send, embeds_ref, product_ref, grad_ref, gate_ref, flat, sems, out_sems = refs
    count = 11
    loaded = refs[-count:]
    placement, arrived = refs[-count - 2 : -count]
    kept_out, moved_out, send_hbm = refs[-count - 5 : -count - 2]
    sources = refs[: -count - 5]
    tab = arrived.shape[0]
    labels, senet_in, senet_out, kron_high, kron_low, first_turned, second_turned, last, second, back_high, first = loaded
    tables = pltpu.make_async_copy(placement_hbm, placement, sems.at[count])
    tables.start()
    pieces = [pltpu.make_async_copy(sources[q], arrived.at[q], sems.at[count + 1 + q]) for q in range(tab)]
    for copy in pieces:
        copy.start()
    loads = [pltpu.make_async_copy(sources[tab + i], loaded[i], sems.at[i]) for i in range(count)]
    for copy in loads[:6]:
        copy.start()

    fields = placement.shape[0]
    lanes = arrived.shape[2]
    total = tab * arrived.shape[1]
    width = total // fields
    factor = fields ** -0.5
    chunk = kron_high.shape[0]
    per = chunk // width
    hidden = second.shape[0]
    depth = send.shape[1]
    slots = fields // tab
    rows = 2 * total // tab
    step = min(chunk, rows)
    mine = lax.axis_index("tab")
    core = mine % 2
    tables.wait()
    for q in range(tab):
        pieces[q].wait()
        for i in range(slots):
            spot = pl.multiple_of(placement[(mine ^ q) * slots + i] * width, width)
            embeds_ref[pl.ds(spot, width), :] = arrived[q, i * width : (i + 1) * width, :]

    dense3 = embeds_ref[...].astype(F32).reshape(fields, width, lanes)
    squeeze = jnp.sum(dense3, axis=1) * (1.0 / width)
    for copy in loads[:5]:
        copy.wait()
    for copy in loads[6:]:
        copy.start()
    pre_one = dot(senet_in[...], squeeze, NN, PRECISE)
    act_one = pre_one * jax.nn.sigmoid(pre_one)
    weights = jax.nn.sigmoid(dot(senet_out[...], act_one, TN, PRECISE))
    sum_plain = jnp.zeros((width, lanes), F32)
    sum_scaled = jnp.zeros((width, lanes), F32)
    for f in range(fields):
        one = embeds_ref[f * width : (f + 1) * width, :].astype(F32)
        sum_plain = sum_plain + one
        sum_scaled = sum_scaled + one * weights[f : f + 1, :]
    for g in range(0, total, chunk):
        block = embeds_ref[g : g + chunk, :]
        product = dot(kron_high[...], block) + dot(kron_low[...], block)
        product_ref[g : g + chunk, :] = product
        product3 = product.reshape(per, width, lanes) * factor
        dense = block.astype(F32).reshape(per, width, lanes)
        scale = weights[g // width : g // width + per][:, None, :]
        plain = (product3 * (sum_plain[None] - dense)).reshape(chunk, lanes).astype(BF)
        scaled = (product3 * scale * (sum_scaled[None] - dense * scale)).reshape(chunk, lanes).astype(BF)
        for start, values in ((g, plain), (total + g, scaled)):
            for piece in range(0, chunk, step):
                owner, spot = divmod(start + piece, rows)
                at = owner // 2 * rows + spot
                joined[(owner % 2) ^ core, at : at + step, :] = values[piece : piece + step]
    blocks = [joined[(o % 2) ^ core, o // 2 * rows : (o // 2 + 1) * rows, :] for o in range(tab)]
    loads[5].wait()
    pre_hidden = dot(first_turned[...], jnp.concatenate(blocks, axis=0))
    for copy in loads[6:]:
        copy.wait()
    hidden_one = (pre_hidden * jax.nn.sigmoid(pre_hidden)).astype(BF)
    pre_second = dot(second_turned[...], hidden_one)
    hidden_two = (pre_second * jax.nn.sigmoid(pre_second)).astype(BF)
    hidden_wide = hidden_two.astype(F32)
    last_wide = last[...]
    logits = jnp.sum(last_wide * hidden_wide, axis=0, keepdims=True)
    grad_logit = jax.nn.sigmoid(logits) - labels[pl.ds(mine, 1), :].astype(F32)
    d_last = jnp.sum(hidden_wide * grad_logit, axis=1, keepdims=True)
    d_pre_two = (grad_logit * last_wide * silu_slope(pre_second)).astype(BF)
    flat[:hidden, :] = dot(hidden_one, d_pre_two, NT)
    d_pre_one = (dot(second[...], d_pre_two) * silu_slope(pre_hidden)).astype(BF)
    joined[0, total:, :] = d_pre_one
    joined[1, total:, :] = d_pre_one
    leave_moved = pltpu.make_async_copy(joined.at[1], moved_out, out_sems.at[1])
    leave_moved.start()
    leave_kept = pltpu.make_async_copy(joined.at[0], kept_out, out_sems.at[0])
    leave_kept.start()

    rest_plain = jnp.zeros((width, lanes), F32)
    rest_scaled = jnp.zeros((width, lanes), F32)
    bil = jnp.zeros((chunk, chunk), F32)
    d_weight_parts = []
    for g in range(0, total, chunk):
        d_plain = dot(first[g : g + chunk, :], d_pre_one).reshape(per, width, lanes)
        d_scaled = dot(first[total + g : total + g + chunk, :], d_pre_one).reshape(per, width, lanes)
        block = embeds_ref[g : g + chunk, :]
        dense = block.astype(F32).reshape(per, width, lanes)
        scale = weights[g // width : g // width + per][:, None, :]
        product = product_ref[g : g + chunk, :].reshape(per, width, lanes) * factor
        others_scaled = d_scaled * product
        d_others_plain = d_plain * product
        d_others_scaled = others_scaled * scale
        rest_plain = rest_plain + jnp.sum(d_others_plain, axis=0)
        rest_scaled = rest_scaled + jnp.sum(d_others_scaled, axis=0)
        away_scaled = sum_scaled[None] - dense * scale
        d_product = (d_plain * (sum_plain[None] - dense) + d_scaled * scale * away_scaled) * factor
        direct = d_product.reshape(chunk, lanes).astype(BF)
        bil = bil + dot(block, direct, NT)
        back = dot(back_high[...], direct).reshape(per, width, lanes)
        grad = back - d_others_plain - d_others_scaled * scale
        grad_ref[g : g + chunk, :] = grad.reshape(chunk, lanes)
        d_weight_parts.append(jnp.sum(others_scaled * away_scaled - dense * d_others_scaled, axis=1))
    d_bil = bil[0:width, 0:width]
    for i in range(1, per):
        d_bil = d_bil + bil[i * width : (i + 1) * width, i * width : (i + 1) * width]
    dense3 = embeds_ref[...].astype(F32).reshape(fields, width, lanes)
    d_weights = jnp.concatenate(d_weight_parts, axis=0) + jnp.sum(dense3 * rest_scaled[None], axis=1)
    d_pre_w = d_weights * weights * (1.0 - weights)
    d_out = dot(act_one, d_pre_w, NT, PRECISE)
    d_act = dot(senet_out[...], d_pre_w, NN, PRECISE) * silu_slope(pre_one)
    d_in = dot(d_act, squeeze, NT, PRECISE)
    d_squeeze = dot(senet_in[...], d_act, TN, PRECISE) * (1.0 / width)
    gate_ref[0] = weights
    gate_ref[1] = d_squeeze
    for s in range(fields):
        spot = pl.multiple_of(placement[s] * width, width)
        at = s % slots * width
        grad = grad_ref[pl.ds(spot, width), :] + rest_plain
        grad = grad + (gate_ref[0, pl.ds(placement[s], 1), :] * rest_scaled + gate_ref[1, pl.ds(placement[s], 1), :])
        send[s // slots, at : at + width, :] = grad.astype(BF)
    senet = senet_in.shape[0]
    lines = flat.shape[0] // tab
    columns = [d_in, d_out, d_bil] + [d_last[i : i + senet, :] for i in range(0, hidden, senet)]
    used = sum(c.shape[1] for c in columns)
    flat[hidden:, :] = jnp.zeros((flat.shape[0] - hidden, hidden), F32)
    flat[hidden : hidden + senet, :] = jnp.concatenate(columns + [jnp.zeros((senet, hidden - used), F32)], axis=1)
    high = logits.astype(BF).astype(F32)
    base = slots * width
    spare = jnp.zeros((depth - base - hidden // lanes * lines - 2, lanes), F32)
    for t in range(tab):
        band = flat[t * lines : (t + 1) * lines, :]
        pieces = [band[:, i : i + lanes] for i in range(0, hidden, lanes)] + [high, logits - high, spare]
        send[t, base:, :] = jnp.concatenate(pieces, axis=0).astype(BF)
    leave_send = pltpu.make_async_copy(send, send_hbm, out_sems.at[2])
    leave_send.start()
    leave_kept.wait()
    leave_moved.wait()
    leave_send.wait()


def depth_of(base, lines, hidden, lanes):
    return -(-(base + hidden // lanes * lines + 2) // 16) * 16


def owner_pass(placement, arrived, labels, senet_in, senet_out, kron_high, kron_low, first_turned, second_turned, last, w_second, back_high, w_first):
    tab = len(arrived)
    total, lanes = tab * arrived[0].shape[0], arrived[0].shape[1]
    senet, fields = senet_in.shape
    hidden = w_second.shape[0]
    lines = -(-(hidden + senet) // tab)
    depth = depth_of(total // tab, lines, hidden, lanes)
    pair = jax.ShapeDtypeStruct((total + hidden, lanes), BF)
    operands = (labels, senet_in, senet_out, kron_high, kron_low, first_turned, second_turned, last, w_second, back_high, w_first)
    return pl.pallas_call(
        owner_body,
        out_shape=(pair, pair, pltpu.HBM((tab, depth, lanes), BF)),
        in_specs=[hspec()] * (1 + tab + len(operands)),
        out_specs=(vspec(), vspec(), hspec()),
        scratch_shapes=[
            pltpu.SMEM((fields,), jnp.int32),
            pltpu.VMEM((tab, total // tab, lanes), BF),
            *[pltpu.VMEM(o.shape, o.dtype) for o in operands],
            pltpu.VMEM((2, total + hidden, lanes), BF),
            pltpu.VMEM((tab, depth, lanes), BF),
            pltpu.VMEM((total, lanes), BF),
            pltpu.VMEM((total, lanes), F32),
            pltpu.VMEM((total, lanes), F32),
            pltpu.VMEM((2, fields, lanes), F32),
            pltpu.VMEM((lines * tab, hidden), F32),
            pltpu.SemaphoreType.DMA((len(operands) + 1 + tab,)),
            pltpu.SemaphoreType.DMA((3,)),
        ],
        compiler_params=params(24),
        name="owner_pass",
    )(*far(placement), *arrived, *far(*operands))


def first_body(kept, came, *outs):
    chips = len(outs)
    rows, _ = outs[0].shape
    chip = lax.axis_index("tab") // 2
    right = jnp.concatenate([kept[chips * rows :, :], came[chips * rows :, :]], axis=1)
    for q in range(chips):
        part = pl.ds(pl.multiple_of((chip ^ q) * rows, rows), rows)
        left = jnp.concatenate([kept[part, :], came[part, :]], axis=1)
        outs[q][...] = dot(left, right, NT).astype(BF)


def first_grad(kept, came, chips, hidden):
    rows = (kept.shape[0] - hidden) // chips
    return pl.pallas_call(
        first_body,
        out_shape=tuple(jax.ShapeDtypeStruct((rows, hidden), BF) for _ in range(chips)),
        in_specs=[vspec()] * 2,
        out_specs=tuple(vspec() for _ in range(chips)),
        compiler_params=params(8),
        name="first_grad",
    )(kept, came)


def proj_body(
    widths_hbm, placement_hbm, pooled, grads_any, route_hbm, summed_out, scores,
    widths, placement, rows_in, grads, route, sems, in_sems, *, line,
):
    slots, _, padded = rows_in.shape
    tab, _, owner = grads.shape
    mine = lax.axis_index("tab")
    first = mine * slots
    pairs = ((grads_any, grads), (placement_hbm, placement), (widths_hbm, widths), (route_hbm, route))
    copies = [pltpu.make_async_copy(source, target, sems.at[i]) for i, (source, target) in enumerate(pairs)]
    large = [pltpu.make_async_copy(pooled.at[s], rows_in.at[s], in_sems.at[s]) for s in range(slots)]
    for copy in copies + large:
        copy.start()
    for copy in copies:
        copy.wait()
    total = line[0]
    width = total // slots
    small = grads[0, total:, :].astype(F32)
    for o in range(1, tab):
        small = small + grads[o, total:, :].astype(F32)
    summed_out[total:, :] = small.astype(BF)
    wanted = route[pl.ds(mine, 1), :]
    spot = lax.broadcasted_iota(jnp.int32, (owner, owner), 0)
    found = jnp.zeros((2, owner), F32)
    for o in range(tab):
        found = found + dot(grads[o, line[1] : line[1] + 2, :], (spot + o * owner == wanted).astype(F32).astype(BF))
    scores[...] = found[0:1] + found[1:2]
    lane = lax.broadcasted_iota(jnp.int32, (width, padded), 1)
    for s in range(slots):
        left = jnp.concatenate([grads[o, s * width : (s + 1) * width, :] for o in range(tab)], axis=1)
        keep = lane < widths[placement[first + s]]
        large[s].wait()
        summed_out[s * width : (s + 1) * width, :] = jnp.where(keep, dot(left, rows_in[s]), 0.0).astype(BF)


def proj_grad(widths, placement, pooled, grads, route, total, line):
    slots, _, padded = pooled.shape
    fields = placement.shape[0]
    _, depth, owner = grads.shape
    return pl.pallas_call(
        functools.partial(proj_body, line=(total, line)),
        out_shape=(jax.ShapeDtypeStruct((depth, padded), BF), jax.ShapeDtypeStruct((1, owner), F32)),
        in_specs=[hspec()] * 5,
        out_specs=(vspec(), vspec()),
        scratch_shapes=[
            pltpu.SMEM((fields,), jnp.int32),
            pltpu.SMEM((fields,), jnp.int32),
            pltpu.VMEM(pooled.shape, BF),
            pltpu.VMEM(grads.shape, BF),
            pltpu.VMEM(route.shape, jnp.int32),
            pltpu.SemaphoreType.DMA((4,)),
            pltpu.SemaphoreType.DMA((slots,)),
        ],
        compiler_params=params(8),
        name="proj_grad",
    )(*far(widths, placement, pooled), grads, *far(route))


def pooled_body(weight_hbm, grads_any, d_pooled, weight, grads, made, spread, sems, out_sems):
    slots, _, padded = made.shape
    tab, total, owner = grads.shape
    width = total // slots
    copies = [
        pltpu.make_async_copy(weight_hbm, weight, sems.at[0]),
        pltpu.make_async_copy(grads_any.at[:, pl.ds(0, total), :], grads, sems.at[1]),
    ]
    for copy in copies:
        copy.start()
    spread[...] = jnp.zeros(spread.shape, BF)
    copies[0].wait()
    for s in range(slots):
        spread[s * width : (s + 1) * width, s * padded : (s + 1) * padded] = weight[s * width : (s + 1) * width, :]
    copies[1].wait()
    gone = []
    for o in range(tab):
        part = slice(o * owner, (o + 1) * owner)
        back = dot(grads[o], spread[...], TN).astype(BF)
        for s in range(slots):
            made[s, part, :] = back[:, s * padded : (s + 1) * padded]
        copy = pltpu.make_async_copy(made.at[:, part, :], d_pooled.at[:, part, :], out_sems.at[o])
        copy.start()
        gone.append(copy)
    for copy in gone:
        copy.wait()


def pooled_grad(pooled, weight, grads):
    slots, _, padded = pooled.shape
    total = weight.shape[0]
    tab, _, owner = grads.shape
    return pl.pallas_call(
        pooled_body,
        out_shape=pltpu.HBM(pooled.shape, BF),
        in_specs=[hspec()] * 2,
        out_specs=hspec(),
        scratch_shapes=[
            pltpu.VMEM(weight.shape, BF),
            pltpu.VMEM((tab, total, owner), BF),
            pltpu.VMEM(pooled.shape, BF),
            pltpu.VMEM((total, slots * padded), BF),
            pltpu.SemaphoreType.DMA((2,)),
            pltpu.SemaphoreType.DMA((tab,)),
        ],
        compiler_params=params(8),
        name="pooled_grad",
    )(*far(weight), grads)


def rep_body(*refs):
    parts, (d_proj, small) = refs[:-2], refs[-2:]
    total = d_proj.shape[0]
    summed = parts[0][...].astype(F32)
    for part in parts[1:]:
        summed = summed + part[...].astype(F32)
    d_proj[...] = summed[:total]
    lines = summed[total:].astype(BF)
    for t in range(small.shape[0]):
        small[t] = lines


def rep_sums(parts, total, tab):
    depth, lanes = parts[0].shape
    return pl.pallas_call(
        rep_body,
        out_shape=(
            jax.ShapeDtypeStruct((total, lanes), F32),
            jax.ShapeDtypeStruct((tab, depth - total, lanes), BF),
        ),
        in_specs=[vspec()] * len(parts),
        out_specs=(vspec(), vspec()),
        compiler_params=params(4),
        name="rep_sums",
    )(*parts)


def unpack_body(arrived, d_second, d_in, d_out, d_bil, d_last, flat):
    tab, _, lanes = arrived.shape
    hidden = d_second.shape[0]
    lines = flat.shape[0] // tab
    for t in range(tab):
        block = arrived[t].astype(F32)
        for i in range(hidden // lanes):
            flat[t * lines : (t + 1) * lines, i * lanes : (i + 1) * lanes] = block[i * lines : (i + 1) * lines]
    d_second[...] = flat[:hidden, :]
    senet, fields = d_in.shape
    width = d_bil.shape[0]
    band = flat[hidden : hidden + senet, :]
    d_in[...] = band[:, :fields]
    d_out[...] = band[:, fields : 2 * fields]
    d_bil[...] = band[:width, 2 * fields : 2 * fields + width]
    column = 2 * fields + width
    pieces = jnp.concatenate([band[:, column + i : column + i + 1] for i in range(hidden // senet)], axis=0)
    row = lax.broadcasted_iota(jnp.int32, (hidden, hidden), 0)
    across = lax.broadcasted_iota(jnp.int32, (hidden, hidden), 1)
    d_last[...] = jnp.sum(jnp.where(row == across, pieces, 0.0), axis=0, keepdims=True)


def unpack(arrived, hidden, senet, fields, width):
    tab = arrived.shape[0]
    lines = -(-(hidden + senet) // tab)
    shapes = ((hidden, hidden), (senet, fields), (senet, fields), (width, width), (1, hidden))
    return pl.pallas_call(
        unpack_body,
        out_shape=tuple(jax.ShapeDtypeStruct(s, F32) for s in shapes),
        in_specs=[vspec()],
        out_specs=tuple(vspec() for _ in shapes),
        scratch_shapes=[pltpu.VMEM((lines * tab, hidden), F32)],
        compiler_params=params(4),
        name="unpack",
    )(arrived)


def embeds_order(tab):
    return range(1, tab)


def swap(x, axis, size, bit):
    return lax.ppermute(x, axis, [(i, i ^ bit) for i in range(size)])


def shards(pooled, widths, placement, route, labels, proj, senet_in, senet_out, bilinear, w_first, w_second, w_last):
    tab = lax.axis_size("tab")
    rep = lax.axis_size("rep")
    rep_index = lax.axis_index("rep")
    slots, rep_rows, padded = pooled.shape
    fields, senet = senet_in.shape
    width = proj.shape[2]
    owner = rep_rows // tab
    hidden = w_second.shape[0]
    chips = tab // 2

    weight, *local = embed_slots(widths, placement, pooled, proj.transpose(0, 2, 1), tab)
    arrived = [local[0]] + [swap(local[q], "tab", tab, q) for q in embeds_order(tab)]
    first_turned, second_turned, kron_high, kron_low, back_high, last_column = prepare(
        weight, w_first, w_second, bilinear, w_last.reshape(1, hidden)
    )
    kept, moved, send = owner_pass(
        placement, arrived, labels.reshape(tab, owner), senet_in.T, senet_out, kron_high, kron_low,
        first_turned, second_turned, last_column, w_second, back_high, w_first,
    )
    came = swap(moved, "tab", tab, 1)
    grads = lax.all_to_all(send, "tab", 0, 0, tiled=True)
    parts = first_grad(kept, came, chips, hidden)
    rows = parts[0].shape[0]
    sent = [swap(parts[q], "tab", tab, 2 * q) for q in range(1, chips)]

    base = slots * width
    line = base + hidden // owner * -(-(hidden + senet) // tab)
    summed, scores = proj_grad(widths, placement, pooled, grads, route.reshape(tab, owner), base, line)
    sums = [summed] + [swap(summed, "rep", rep, q) for q in range(1, rep)]
    d_pooled = pooled_grad(pooled, weight, grads)
    d_proj, small = rep_sums(sums, base, tab)
    d_proj = d_proj.reshape(slots, width, padded).transpose(0, 2, 1)
    small = lax.all_to_all(small, "tab", 0, 0, tiled=True)
    g_second, g_in, g_out, g_bil, g_last = unpack(small, hidden, senet, fields, width)

    first_sum = parts[0].astype(F32)
    for part in sent:
        first_sum = first_sum + part.astype(F32)
    low_bit = rep_index % 2
    halves = first_sum.astype(BF).reshape(2, rows // 2, hidden)
    mine = lax.dynamic_index_in_dim(halves, low_bit, 0, keepdims=False)
    theirs = lax.dynamic_index_in_dim(halves, 1 - low_bit, 0, keepdims=False)
    theirs = swap(theirs, "rep", rep, 1)
    mine = (mine.astype(F32) + theirs.astype(F32)).astype(BF)
    bit = 2
    while bit < rep:
        theirs = swap(mine, "rep", rep, bit)
        mine = (mine.astype(F32) + theirs.astype(F32)).astype(BF)
        bit *= 2
    back = swap(mine, "rep", rep, 1)
    d_first = jnp.where(
        low_bit == 0, jnp.concatenate([mine, back], axis=0), jnp.concatenate([back, mine], axis=0)
    ).astype(F32)
    return (
        scores, d_pooled, d_proj, g_in.T, g_out, g_bil, d_first, g_second, g_last.reshape(hidden),
    )


def solution(mesh):
    placed = (
        P("tab", "rep", None), P(), P(), P("rep", None), P("rep", None),
        P(), P(), P(), P(), P(), P(), P(),
    )
    return jax.shard_map(
        shards,
        mesh=mesh,
        in_specs=placed,
        out_specs=(P("rep", "tab"), P("tab", "rep", None), P("tab", None, None), P(), P(), P(), P("tab", None), P(), P()),
        check_vma=False,
    )
```
